128 devices in a mesh: grp: 16 (over y, x), col: 8 (over z, core).
Axes of the slice: x: 4, y: 4, z: 4, core: 2. Of those that a mesh axis runs over, the one named last changes fastest.
Arguments:
- front: float32 [16384, 16384], P(None, ('grp', 'col')), as said below
- contributions: float32 [16, 1024, 1024], P('grp', None, 'col')
- block_map: int32 [16, 8], P('grp'), may hold values from 0 to 127, as said below
- pivot_flags: int32 [16384], P(('grp', 'col')), may hold values 0 or 1
Outputs:
- factored: float32 [16384, 16384], P(None, ('grp', 'col'))
The draws below stay inside these ranges and needn't reach their ends.
Inputs may be any that keep to these rules, and one draw needn't show every extreme that they name: `block_map`: within each child the 8 entries are distinct, and entry j leaves the remainder j when divided by 8. The assembled front is symmetric positive definite.
All inputs are finite; a program needn't handle non-finite values. No bound on the sum of `pivot_flags` on one device may be relied on, other than what follows from the above.
Results may differ from the reference program's by a relative error of at most 0.005.
Values may be sent and summed in bfloat16 or wider, within the bound.
A program may use at most 192 MiB of HBM per device.

```python
import jax
import jax.numpy as jnp
from jax import lax

BLOCK = 128
PANELS = 4
RBC = 1
GROUPS = 16
RB = 8
CHILD = 1024
ORDER = 16384
PWIDTH = 512
N_GRP = 16
N_COL = 8


def draw_front(key, part):
    first = jax.random.fold_in(key, 11)
    second = jax.random.fold_in(key, 12)
    fourth = jax.random.fold_in(key, 14)
    noise = jax.random.normal(first, (ORDER, ORDER), jnp.float32)
    matrix = (noise + noise.T) * (0.5 / jnp.sqrt(2.0 * ORDER))
    diag_part = jax.random.uniform(second, (ORDER,), jnp.float32, 2.0, 4.0)
    matrix = matrix + jnp.diag(diag_part)
    coupling = jax.random.normal(fourth, (ORDER, PWIDTH), jnp.float32) / jnp.sqrt(1.0 * PWIDTH)
    row_index = jnp.arange(ORDER, dtype=jnp.int32)
    row_weight = jnp.where(row_index < PWIDTH, 3.0, 1.5).astype(jnp.float32)
    coupling = coupling * row_weight[:, None]
    matrix = matrix + jnp.dot(coupling, coupling.T, precision=lax.Precision.HIGHEST)
    return matrix


def draw_contributions(key, part):
    first = jax.random.fold_in(key, 21)
    factor = jax.random.normal(first, (N_GRP, CHILD, CHILD), jnp.float32)
    blocks = jnp.einsum('gij,gkj->gik', factor, factor) * (0.5 / CHILD)
    return blocks


def draw_block_map(key, part):
    keys = jax.random.split(jax.random.fold_in(key, 31), N_GRP * N_COL)
    perms = jax.vmap(lambda single: jax.random.permutation(single, N_GRP))(keys)[:, :RBC]
    perms = perms.reshape(N_GRP, N_COL, RBC)
    residue = jnp.arange(N_COL, dtype=jnp.int32)[None, :, None]
    return (N_COL * perms.astype(jnp.int32) + residue).reshape(N_GRP, RB).astype(jnp.int32)


def set_ends(array, rng, least, largest):
    shape = array.shape
    place = [jax.random.randint(jax.random.fold_in(rng, axis), (), 0, shape[axis]) for axis in range(len(shape))]
    array = array.at[tuple(place)].set(least)
    longest = shape.index(max(shape))
    place[longest] = (place[longest] + 1) % shape[longest]
    return array.at[tuple(place)].set(largest)


def setup_inputs(seed: int = 0) -> dict:
    arg_keys = jax.random.split(jax.random.key(seed), 5)
    return {
        "front": draw_front(jax.random.fold_in(arg_keys[4], 71), 0),
        "contributions": draw_contributions(jax.random.fold_in(arg_keys[4], 71), 0),
        "block_map": draw_block_map(jax.random.fold_in(arg_keys[4], 71), 0),
        "pivot_flags": set_ends((jax.random.randint(arg_keys[3], (ORDER,), 0, 4) < 1).astype(jnp.int32), jax.random.fold_in(arg_keys[3], 1), 0, 1),
    }


def factor_panel(column, earlier, pivots, step, width):
    if step > 0:
        rows = earlier[step * width:(step + 1) * width].astype(jnp.float32) * pivots.astype(jnp.float32)[None, :]
        coef = rows.astype(jnp.bfloat16)
        column = column - jnp.dot(earlier.astype(jnp.float32), coef.astype(jnp.float32).T, precision=lax.Precision.HIGHEST)
    block = column[step * width:(step + 1) * width]
    chol = jnp.linalg.cholesky(block)
    cdiag = jnp.diagonal(chol)
    below = column[(step + 1) * width:]
    lower = lax.linalg.triangular_solve(chol, below, left_side=False, lower=True, transpose_a=True) / cdiag[None, :]
    unit = chol / cdiag[None, :]
    upper = jnp.zeros((step * width, width), jnp.float32)
    panel = jnp.concatenate([upper, unit, lower], axis=0).astype(jnp.bfloat16)
    return (panel, (cdiag * cdiag).astype(jnp.bfloat16))

def reference(front, contributions, block_map, pivot_flags):
    order = front.shape[0]
    blocks = order // BLOCK
    rb = block_map.shape[1]
    tiles = front.reshape(blocks, BLOCK, blocks, BLOCK)
    for group in range(GROUPS):
        index = block_map[group]
        piece = contributions[group].reshape(rb, BLOCK, rb, BLOCK).transpose(0, 2, 1, 3)
        tiles = tiles.at[index[:, None], :, index[None, :], :].add(piece)
    assembled = tiles.reshape(order, order)
    diag_index = jnp.arange(order, dtype=jnp.int32)
    assembled = assembled.at[diag_index, diag_index].add(pivot_flags.astype(jnp.float32))
    panels = []
    pivots = []
    for step in range(PANELS):
        column = assembled[:, step * BLOCK:(step + 1) * BLOCK]
        if step > 0:
            earlier = jnp.concatenate(panels, axis=1)
            before = jnp.concatenate(pivots)
        else:
            earlier = jnp.zeros((order, 0), jnp.bfloat16)
            before = jnp.zeros((0,), jnp.bfloat16)
        panel, piv = factor_panel(column, earlier, before, step, BLOCK)
        panels.append(panel)
        pivots.append(piv)
    all_l = jnp.concatenate(panels, axis=1)
    all_d = jnp.concatenate(pivots)
    pw = PANELS * BLOCK
    lrest = all_l[pw:].astype(jnp.float32)
    wrest = (lrest * all_d.astype(jnp.float32)[None, :]).astype(jnp.bfloat16)
    trailing = assembled[pw:, pw:] - jnp.dot(lrest, wrest.astype(jnp.float32).T, precision=lax.Precision.HIGHEST)
    right = jnp.concatenate([jnp.zeros((pw, order - pw), jnp.float32), trailing], axis=0)
    return jnp.concatenate([all_l.astype(jnp.float32), right], axis=1)
```

```python
import functools

import jax
import jax.numpy as jnp
from jax import lax
from jax.experimental import pallas as pl
from jax.experimental.pallas import tpu as pltpu
from jax.sharding import PartitionSpec as P

PANELS = 4
W = 128
LEAD = PANELS * W
PACK = 16
F32 = jnp.float32
BF16 = jnp.bfloat16


def ldl_inverse(m_ref, d_ref):
    lane = lax.broadcasted_iota(jnp.int32, (8, W), 1)
    sub = lax.broadcasted_iota(jnp.int32, (8, W), 0)
    for g in range(W // 8):
        c0 = 8 * g
        rest = W - c0 - 8
        top = m_ref[c0 : c0 + 8, :]
        ctop = [jnp.broadcast_to(top[:, c0 + j : c0 + j + 1], (8, W)) for j in range(8)]
        if rest:
            low = m_ref[c0 + 8 :, :]
            clow = [jnp.broadcast_to(low[:, c0 + j : c0 + j + 1], (rest, W)) for j in range(8)]
        inside = (lane >= c0) & (lane < c0 + 8)
        rows = jnp.where(inside, (lane == sub + c0).astype(F32), top)
        dvec = jnp.zeros((8, W), F32)
        llow = []
        for j in range(8):
            piv = ctop[j][j : j + 1, :]
            rec = 1.0 / piv
            dvec = jnp.where(sub == j, piv, dvec)
            lt = jnp.where(sub > j, ctop[j] * rec, 0.0)
            ups = [ctop[jj][j : j + 1, :] for jj in range(j + 1, 8)]
            for jj, up in zip(range(j + 1, 8), ups):
                ctop[jj] = ctop[jj] - lt * up
            rows = rows - lt * rows[j : j + 1, :]
            if rest:
                ll = clow[j] * rec
                for jj, up in zip(range(j + 1, 8), ups):
                    clow[jj] = clow[jj] - ll * up
                llow.append(ll)
        m_ref[c0 : c0 + 8, :] = rows
        d_ref[c0 : c0 + 8, :] = dvec
        if rest:
            lanes = lax.broadcasted_iota(jnp.int32, (rest, W), 1)
            acc = jnp.where((lanes >= c0) & (lanes < c0 + 8), 0.0, low)
            for j in range(8):
                acc = acc - llow[j] * rows[j : j + 1, :]
            m_ref[c0 + 8 :, :] = acc


def factor_kernel(me_ref, lead_ref, own_ref, l_ref, w_ref, t_ref, m_ref, d_ref):
    me = me_ref[0]
    row = lax.broadcasted_iota(jnp.int32, (W, W), 0)
    col = lax.broadcasted_iota(jnp.int32, (W, W), 1)
    t_ref[:, :LEAD] = lead_ref[...]
    t_ref[:, LEAD:] = own_ref[...]

    def step(k, carry):
        here = pl.ds(pl.multiple_of(k * W, W), W)
        diag = t_ref[here, here]
        diag = 0.5 * (diag + diag.T)
        m_ref[...] = diag
        ldl_inverse(m_ref, d_ref)
        d = d_ref[...]
        minv = jnp.where(col <= row, m_ref[...], 0.0) / d
        piv = d.astype(BF16).astype(F32)
        t = t_ref[here, :]
        own = jnp.where(me == k, diag, t[:, LEAD:])
        q = jnp.dot(
            minv,
            jnp.concatenate([t[:, :LEAD], own], axis=1),
            precision=lax.Precision.HIGHEST,
            preferred_element_type=F32,
        )
        q_own = q[:, LEAD:]
        q_own = jnp.where((me > k) | ((me == k) & (col >= row)), q_own, 0.0)
        q_own = q_own.astype(BF16).astype(F32)
        q_lead = q[:, :LEAD].astype(BF16)
        pw = jnp.concatenate([piv] * PANELS, axis=1)
        coef = (q_lead.astype(F32) * pw).astype(BF16).astype(F32).T.astype(BF16)
        t_ref[...] = t_ref[...] - jnp.dot(
            coef,
            jnp.concatenate([q_lead, q_own.astype(BF16)], axis=1),
            preferred_element_type=F32,
        )
        l_ref[:, here] = q_own.T.astype(BF16)
        w_ref[here, :] = (q_own * piv).astype(BF16)
        return carry

    lax.fori_loop(0, PANELS, step, 0)


def factor(me, lead, own):
    return pl.pallas_call(
        factor_kernel,
        out_shape=(
            jax.ShapeDtypeStruct((W, LEAD), BF16),
            jax.ShapeDtypeStruct((LEAD, W), BF16),
        ),
        in_specs=[
            pl.BlockSpec(memory_space=pltpu.SMEM),
            pl.BlockSpec(memory_space=pltpu.VMEM),
            pl.BlockSpec(memory_space=pltpu.VMEM),
        ],
        out_specs=(pl.BlockSpec(memory_space=pltpu.VMEM), pl.BlockSpec(memory_space=pltpu.VMEM)),
        scratch_shapes=[
            pltpu.VMEM((LEAD, LEAD + W), F32),
            pltpu.VMEM((W, W), F32),
            pltpu.VMEM((W, W), F32),
        ],
        name="factor",
    )(me, lead, own)


CHUNK = 1024


def update_kernel(me_ref, maps_ref, front_ref, l_ref, w_ref, parts_ref, flag_ref, out_ref, list_ref):
    s = pl.program_id(0)
    me = me_ref[0]
    groups = maps_ref.shape[0]

    @pl.when(s == 0)
    def _():
        count = jnp.int32(0)
        for g in range(groups):
            mine = maps_ref[g, lax.rem(me, 8)] == me
            list_ref[count] = g
            count = count + mine.astype(jnp.int32)
        list_ref[groups] = count

    @pl.when(me < PANELS)
    def _():
        out_ref[...] = l_ref[:, pl.ds(pl.multiple_of(jnp.minimum(me, PANELS - 1) * W, W), W)].astype(F32)

    @pl.when(me >= PANELS)
    def _():
        out_ref[...] = front_ref[...] - jnp.dot(l_ref[...], w_ref[...], preferred_element_type=F32)

        def add(n, carry):
            g = list_ref[n]
            for i in range(CHUNK // W):

                @pl.when(maps_ref[g, i] == s * (CHUNK // W) + i)
                def _():
                    out_ref[i * W : (i + 1) * W, :] += parts_ref[g, i * W : (i + 1) * W, :].astype(F32)

            return carry

        lax.fori_loop(0, list_ref[groups], add, 0)

        @pl.when(lax.div(me, CHUNK // W) == s)
        def _():
            at = pl.ds(pl.multiple_of(lax.rem(me, CHUNK // W) * W, W), W)
            row = lax.broadcasted_iota(jnp.int32, (W, W), 0)
            col = lax.broadcasted_iota(jnp.int32, (W, W), 1)
            out_ref[at, :] += jnp.where(row == col, flag_ref[...].astype(F32), 0.0)

        @pl.when(s == 0)
        def _():
            out_ref[:LEAD, :] = jnp.zeros((LEAD, W), F32)


def update(me, maps, front, all_l, w, parts, flags):
    order = front.shape[0]
    groups = parts.shape[0]
    return pl.pallas_call(
        update_kernel,
        out_shape=jax.ShapeDtypeStruct((order, W), F32),
        grid=(order // CHUNK,),
        in_specs=[
            pl.BlockSpec(memory_space=pltpu.SMEM),
            pl.BlockSpec(memory_space=pltpu.SMEM),
            pl.BlockSpec((CHUNK, W), lambda s: (s, 0)),
            pl.BlockSpec((CHUNK, LEAD), lambda s: (s, 0)),
            pl.BlockSpec((LEAD, W), lambda s: (0, 0)),
            pl.BlockSpec(parts.shape, lambda s: (0, 0, 0)),
            pl.BlockSpec((1, W), lambda s: (0, 0)),
        ],
        out_specs=pl.BlockSpec((CHUNK, W), lambda s: (s, 0)),
        scratch_shapes=[pltpu.SMEM((groups + 1,), jnp.int32)],
        name="update",
    )(me, maps, front, all_l, w, parts, flags)


def on_device(front, contributions, block_map, pivot_flags):
    both = ("grp", "col")
    me = lax.axis_index(both)
    flags = pivot_flags.reshape(1, W)
    child = contributions.shape[1]
    packed = jnp.concatenate(
        [
            contributions[0].astype(BF16),
            jnp.pad(block_map.astype(BF16), ((0, PACK - 1), (0, W - block_map.shape[1]))),
        ],
        axis=0,
    )
    got = lax.all_gather(packed, "grp", axis=0)
    parts = got[:, :child]
    maps = got[:, child, : block_map.shape[1]].astype(jnp.int32)
    mine = lax.dynamic_index_in_dim(maps, lax.axis_index("col"), 1, keepdims=False) == me
    hit = maps[:, :PANELS] == jnp.arange(PANELS, dtype=jnp.int32)[None, :]
    weight = (mine[:, None] & hit).astype(F32)
    added = jnp.sum(
        got[:, :LEAD].reshape(-1, PANELS, W, W).astype(F32) * weight[:, :, None, None], axis=0
    ).reshape(LEAD, W)
    at = jnp.arange(LEAD, dtype=jnp.int32)[:, None] == me * W + jnp.arange(W, dtype=jnp.int32)[None, :]
    own = front[:LEAD] + added + jnp.where(at, flags.astype(F32), 0.0)
    lead = jnp.stack([jnp.where(me == k, own, 0.0) for k in range(PANELS)], axis=1).reshape(LEAD, LEAD)
    lead = lax.psum(lead, both)
    which = me.reshape(1)
    own_l, own_w = factor(which, lead, own)
    all_l = lax.all_gather(own_l, both, axis=0, tiled=True)
    return update(which, maps, front, all_l, own_w, parts, flags)


def solution(mesh):
    return jax.shard_map(
        on_device,
        mesh=mesh,
        in_specs=(
            P(None, ("grp", "col")),
            P("grp", None, "col"),
            P("grp", None),
            P(("grp", "col")),
        ),
        out_specs=P(None, ("grp", "col")),
        check_vma=False,
    )
```

```python
import functools

import jax
import jax.numpy as jnp
from jax import lax
from jax.experimental import pallas as pl
from jax.experimental.pallas import tpu as pltpu
from jax.sharding import PartitionSpec as P

PANELS = 4
W = 128
LEAD = PANELS * W
PACK = 16
MESH = pl.DeviceIdType.MESH
FULL = pl.ds(0, 4)
F32 = jnp.float32
BF16 = jnp.bfloat16


def ldl_inverse(m_ref, d_ref):
    lane = lax.broadcasted_iota(jnp.int32, (8, W), 1)
    sub = lax.broadcasted_iota(jnp.int32, (8, W), 0)
    for g in range(W // 8):
        c0 = 8 * g
        rest = W - c0 - 8
        top = m_ref[c0 : c0 + 8, :]
        ctop = [jnp.broadcast_to(top[:, c0 + j : c0 + j + 1], (8, W)) for j in range(8)]
        if rest:
            low = m_ref[c0 + 8 :, :]
            clow = [jnp.broadcast_to(low[:, c0 + j : c0 + j + 1], (rest, W)) for j in range(8)]
        inside = (lane >= c0) & (lane < c0 + 8)
        rows = jnp.where(inside, (lane == sub + c0).astype(F32), top)
        dvec = jnp.zeros((8, W), F32)
        llow = []
        for j in range(8):
            piv = ctop[j][j : j + 1, :]
            rec = 1.0 / piv
            dvec = jnp.where(sub == j, piv, dvec)
            lt = jnp.where(sub > j, ctop[j] * rec, 0.0)
            ups = [ctop[jj][j : j + 1, :] for jj in range(j + 1, 8)]
            for jj, up in zip(range(j + 1, 8), ups):
                ctop[jj] = ctop[jj] - lt * up
            rows = rows - lt * rows[j : j + 1, :]
            if rest:
                ll = clow[j] * rec
                for jj, up in zip(range(j + 1, 8), ups):
                    clow[jj] = clow[jj] - ll * up
                llow.append(ll)
        m_ref[c0 : c0 + 8, :] = rows
        d_ref[c0 : c0 + 8, :] = dvec
        if rest:
            lanes = lax.broadcasted_iota(jnp.int32, (rest, W), 1)
            acc = jnp.where((lanes >= c0) & (lanes < c0 + 8), 0.0, low)
            for j in range(8):
                acc = acc - llow[j] * rows[j : j + 1, :]
            m_ref[c0 + 8 :, :] = acc


class Place:
    def __init__(self):
        self.g = lax.axis_index("grp")
        self.c = lax.axis_index("col")
        self.at = {"x": lax.rem(self.g, 4), "y": lax.div(self.g, 4), "z": lax.div(self.c, 2)}
        self.core = lax.rem(self.c, 2)
        self.partner = (self.g, self.at["z"] * 2 + 1 - self.core)

    def near(self, dim, delta):
        to = dict(self.at)
        to[dim] = lax.rem(self.at[dim] + delta + 4, 4)
        return (to["y"] * 4 + to["x"], to["z"] * 2 + self.core)

    def greet(self):
        barrier = pltpu.get_barrier_semaphore()
        peers = [self.near(d, s) for d in "xyz" for s in (1, -1)] + [self.partner]
        for peer in peers:
            pl.semaphore_signal(barrier, inc=1, device_id=peer, device_id_type=MESH)
        pl.semaphore_wait(barrier, len(peers))


class Wires:
    def __init__(self, send, recv, count):
        self.send, self.recv, self.count, self.used = send, recv, count, 0

    def copy(self, ref, device):
        n = self.used
        self.used += 1
        assert n < self.count
        return pltpu.make_async_remote_copy(
            src_ref=ref,
            dst_ref=ref,
            send_sem=self.send.at[n],
            recv_sem=self.recv.at[n],
            device_id=device,
            device_id_type=MESH,
        )


def gather_stream(place, wires, view, order, rows, middle, across):
    lo, hi = pl.ds(rows[0], middle - rows[0]), pl.ds(middle, rows[1] - middle)
    every = pl.ds(rows[0], rows[1] - rows[0])
    sent = []
    d2d = []

    def launch(copy, to=None):
        copy.start()
        sent.append(copy)
        if to is not None:
            to.append(copy)
        return copy

    for phase, dim in enumerate(order):
        last = across and phase == len(order) - 1

        def unit(v, r, dim=dim, phase=phase):
            where = {d: (FULL if d in order[:phase] else place.at[d]) for d in order}
            where[dim] = v
            return view(where, r)

        mine = place.at[dim]
        before, after, far = (lax.rem(mine + n, 4) for n in (3, 1, 2))
        right, left = place.near(dim, 1), place.near(dim, -1)
        to_right = launch(wires.copy(unit(mine, every), right))
        to_left = launch(wires.copy(unit(mine, every), left))
        if last:
            launch(wires.copy(unit(mine, every), place.partner), d2d)
        yield
        to_right.wait_recv()
        on_right = launch(wires.copy(unit(before, lo), right))
        if last:
            launch(wires.copy(unit(before, every), place.partner), d2d)
        to_left.wait_recv()
        on_left = launch(wires.copy(unit(after, hi), left))
        if last:
            launch(wires.copy(unit(after, every), place.partner), d2d)
        yield
        on_right.wait_recv()
        on_left.wait_recv()
        if last:
            launch(wires.copy(unit(far, every), place.partner), d2d)
    yield
    for copy in d2d:
        copy.wait_recv()
    for copy in sent:
        copy.wait_send()


def ring_bcast(on, r, wires, whole, lo, hi, right, left, partner=None, other=None):
    to_right, to_left = wires.copy(whole, right), wires.copy(whole, left)
    on_right, on_left = wires.copy(lo, right), wires.copy(hi, left)
    across = wires.copy(whole, partner) if partner is not None else None

    @pl.when(on & (r == 0))
    def _():
        to_right.start()
        to_left.start()
        if across is not None:
            across.start()

    yield

    @pl.when(on & (r == 1))
    def _():
        to_right.wait_recv()
        on_right.start()
        if across is not None:
            across.start()

    @pl.when(on & (r == 3))
    def _():
        to_left.wait_recv()
        on_left.start()
        if across is not None:
            across.start()

    yield

    @pl.when(on & (r == 2))
    def _():
        on_right.wait_recv()
        on_left.wait_recv()
        if across is not None:
            across.start()

    yield "got"
    if across is not None:

        @pl.when(other)
        def _():
            across.wait_recv()

        @pl.when(on)
        def _():
            across.wait_send()

    @pl.when(on & (r == 0))
    def _():
        to_right.wait_send()
        to_left.wait_send()

    @pl.when(on & (r == 1))
    def _():
        on_right.wait_send()

    @pl.when(on & (r == 3))
    def _():
        on_left.wait_send()


def run(*streams):
    streams = list(streams)
    while streams:
        streams = [s for s in streams if next(s, "end") != "end"]


ROWS_A = ((0, 144, 80, "xy"), (144, 272, 208, "yx"), (272, 400, 336, "xy"), (400, 528, 464, "yx"))
ROWS_B = ((528, 656, 592, "xy"), (656, 784, 720, "yx"), (784, 912, 848, "xy"), (912, 1040, 976, "yx"))
WIRES_1 = 146


def exchange_kernel(packed_ref, own_ref, cg_ref, b_ref, lead_ref, flead_ref, load_sem, send_sem, recv_sem):
    place = Place()
    wires = Wires(send_sem, recv_sem, WIRES_1)
    x, y, z = place.at["x"], place.at["y"], place.at["z"]
    me = place.g * 8 + place.c
    load = pltpu.make_async_copy(packed_ref, cg_ref.at[y, x], load_sem.at[0])
    load.start()
    load_lead = pltpu.make_async_copy(own_ref, flead_ref, load_sem.at[1])
    load_own = pltpu.make_async_copy(own_ref, b_ref, load_sem.at[2])
    load_own.start()

    @pl.when(place.g == 0)
    def _():
        load_lead.start()
        load_lead.wait()

    load.wait()
    load_own.wait()
    place.greet()

    def view(where, rows):
        return cg_ref.at[where["y"], where["x"], rows, :]

    def spread(j):
        first, second = ("x", "y") if j % 2 == 0 else ("y", "x")
        base = j * W
        refs = [flead_ref.at[pl.ds(base, W)], flead_ref.at[pl.ds(base, W // 2)], flead_ref.at[pl.ds(base + W // 2, W // 2)]]
        low = place.c < PANELS
        for dim, on in ((first, low & (place.at[second] == 0)), (second, low)):
            yield from ring_bcast(on, place.at[dim], wires, *refs, place.near(dim, 1), place.near(dim, -1))

    def streams(table):
        return [gather_stream(place, wires, view, order, (r0, r1), mid, False) for r0, r1, mid, order in table]

    run(*streams(ROWS_A), *[spread(j) for j in range(PANELS)])
    rest = streams(ROWS_B)
    for s in rest:
        next(s)

    pick = lax.broadcasted_iota(jnp.int32, (PACK, W), 0)
    weights = []
    for g in range(16):
        entry = cg_ref[g // 4, g % 4, 0:PACK, :].astype(F32)
        target = jnp.sum(jnp.where(pick == place.c, entry, 0.0), axis=0, keepdims=True)
        own_hit = target == me.astype(F32)
        lead_hit = target == place.c.astype(F32)
        here = [entry[k : k + 1, :] == float(k) for k in range(PANELS)]
        weights.append(
            (
                [jnp.where(own_hit & h, 1.0, 0.0) for h in here],
                [jnp.where(lead_hit & h, 1.0, 0.0) for h in here],
            )
        )
    for k in range(PANELS):
        at = pl.ds(k * W, W)
        acc_own, acc_lead = b_ref[at, :], flead_ref[at, :]
        for g in range(16):
            block = cg_ref[g // 4, g % 4, PACK + k * W : PACK + (k + 1) * W, :].astype(F32)
            acc_own = acc_own + block * weights[g][0][k]
            acc_lead = acc_lead + block * weights[g][1][k]
        b_ref[at, :] = acc_own
        for l in range(k, PANELS):

            @pl.when(place.c == l)
            def _():
                lead_ref[l, k] = acc_lead

    def lead_unit(l, k):
        on = place.core == l % 2
        r = lax.rem(z - l // 2 + 4, 4)
        refs = [lead_ref.at[l, k], lead_ref.at[l, k, pl.ds(0, W // 2)], lead_ref.at[l, k, pl.ds(W // 2, W // 2)]]
        return ring_bcast(
            on, r, wires, *refs, place.near("z", 1), place.near("z", -1), place.partner, place.core != l % 2
        )

    run(*[lead_unit(l, k) for k in range(PANELS) for l in range(k, PANELS)], *rest)


def exchange(packed, own):
    rows = packed.shape[0]
    vmem = pl.BlockSpec(memory_space=pltpu.VMEM)
    return pl.pallas_call(
        exchange_kernel,
        out_shape=(
            jax.ShapeDtypeStruct((4, 4, rows, W), BF16),
            jax.ShapeDtypeStruct((LEAD, W), F32),
            jax.ShapeDtypeStruct((PANELS, PANELS, W, W), F32),
        ),
        in_specs=[pl.BlockSpec(memory_space=pl.ANY)] * 2,
        out_specs=(vmem, vmem, vmem),
        scratch_shapes=[
            pltpu.VMEM((LEAD, W), F32),
            pltpu.SemaphoreType.DMA((3,)),
            pltpu.SemaphoreType.DMA((WIRES_1,)),
            pltpu.SemaphoreType.DMA((WIRES_1,)),
        ],
        compiler_params=pltpu.CompilerParams(collective_id=0, has_side_effects=True),
        name="exchange",
    )(packed, own)


TILES = (((0, 48), (48, 96), (96, 128)), ((0, 48), (48, 80), (80, 128)), ((0, 32), (32, 80), (80, 128)), ((0, 48), (48, 96), (96, 128)))
ORDERS = ("xyz", "yzx", "zxy")
WIRES_3 = 192


def gather_kernel(l_ref, all_ref, load_sem, send_sem, recv_sem):
    place = Place()
    wires = Wires(send_sem, recv_sem, WIRES_3)
    own = all_ref.at[:, place.at["y"], place.at["x"], place.at["z"], place.core]
    load = pltpu.make_async_copy(l_ref, own, load_sem.at[0])
    load.start()
    load.wait()
    place.greet()

    def stream(k, p):
        def view(where, rows):
            return all_ref.at[k, where["y"], where["x"], where["z"], place.core, rows, :]

        r0, r1 = TILES[k][p]
        half = (r1 - r0) // 32 * 16 if (k + p) % 2 else (r1 - r0 + 16) // 32 * 16
        return gather_stream(place, wires, view, ORDERS[p], (r0, r1), r0 + half, True)

    run(*[stream(k, p) for k in range(PANELS) for p in range(3)])


def gather(own_l):
    return pl.pallas_call(
        gather_kernel,
        out_shape=jax.ShapeDtypeStruct((PANELS, 4, 4, 4, 2, W, W), BF16),
        in_specs=[pl.BlockSpec(memory_space=pl.ANY)],
        out_specs=pl.BlockSpec(memory_space=pltpu.VMEM),
        scratch_shapes=[
            pltpu.SemaphoreType.DMA((1,)),
            pltpu.SemaphoreType.DMA((WIRES_3,)),
            pltpu.SemaphoreType.DMA((WIRES_3,)),
        ],
        compiler_params=pltpu.CompilerParams(collective_id=1, has_side_effects=True),
        name="gather",
    )(own_l)


def factor_kernel(me_ref, lead_ref, own_ref, l_ref, w_ref, t_ref, m_ref, d_ref):
    me = me_ref[0]
    row = lax.broadcasted_iota(jnp.int32, (W, W), 0)
    col = lax.broadcasted_iota(jnp.int32, (W, W), 1)
    for k in range(PANELS):
        for l in range(PANELS):
            t_ref[k * W : (k + 1) * W, l * W : (l + 1) * W] = lead_ref[l, k] if l >= k else jnp.zeros((W, W), F32)
    t_ref[:, LEAD:] = own_ref[...]

    def step(k, carry):
        here = pl.ds(pl.multiple_of(k * W, W), W)
        diag = t_ref[here, here]
        diag = 0.5 * (diag + diag.T)
        m_ref[...] = diag
        ldl_inverse(m_ref, d_ref)
        d = d_ref[...]
        minv = jnp.where(col <= row, m_ref[...], 0.0) / d
        piv = d.astype(BF16).astype(F32)
        t = t_ref[here, :]
        own = jnp.where(me == k, diag, t[:, LEAD:])
        q = jnp.dot(
            minv,
            jnp.concatenate([t[:, :LEAD], own], axis=1),
            precision=lax.Precision.HIGHEST,
            preferred_element_type=F32,
        )
        q_own = q[:, LEAD:]
        q_own = jnp.where((me > k) | ((me == k) & (col >= row)), q_own, 0.0)
        q_own = q_own.astype(BF16).astype(F32)
        q_lead = q[:, :LEAD].astype(BF16)
        pw = jnp.concatenate([piv] * PANELS, axis=1)
        coef = (q_lead.astype(F32) * pw).astype(BF16).astype(F32).T.astype(BF16)
        t_ref[...] = t_ref[...] - jnp.dot(
            coef,
            jnp.concatenate([q_lead, q_own.astype(BF16)], axis=1),
            preferred_element_type=F32,
        )
        l_ref[k] = q_own.T.astype(BF16)
        w_ref[here, :] = (q_own * piv).astype(BF16)
        return carry

    lax.fori_loop(0, PANELS, step, 0)


def factor(me, lead, own):
    return pl.pallas_call(
        factor_kernel,
        out_shape=(
            jax.ShapeDtypeStruct((PANELS, W, W), BF16),
            jax.ShapeDtypeStruct((LEAD, W), BF16),
        ),
        in_specs=[
            pl.BlockSpec(memory_space=pltpu.SMEM),
            pl.BlockSpec(memory_space=pltpu.VMEM),
            pl.BlockSpec(memory_space=pltpu.VMEM),
        ],
        out_specs=(pl.BlockSpec(memory_space=pltpu.VMEM), pl.BlockSpec(memory_space=pltpu.VMEM)),
        scratch_shapes=[
            pltpu.VMEM((LEAD, LEAD + W), F32),
            pltpu.VMEM((W, W), F32),
            pltpu.VMEM((W, W), F32),
        ],
        name="factor",
    )(me, lead, own)


CHUNK = 2048
SPAN = CHUNK // W


def update_kernel(me_ref, maps_ref, front_ref, l_ref, w_ref, parts_ref, flag_ref, out_ref, list_ref, held, sems):
    s = pl.program_id(0)
    me = me_ref[0]
    groups = maps_ref.shape[0]

    def load(g):
        return pltpu.make_async_copy(parts_ref.at[g], held.at[g], sems.at[g])

    @pl.when(s == 0)
    def _():
        count = jnp.int32(0)
        for g in range(groups):
            mine = maps_ref[g, lax.rem(me, 8)] == me
            list_ref[count] = g
            count = count + mine.astype(jnp.int32)

            @pl.when(mine)
            def _():
                load(g).start()

        list_ref[groups] = count

        for g in range(groups):

            @pl.when(maps_ref[g, lax.rem(me, 8)] == me)
            def _():
                load(g).wait()

    @pl.when(me < PANELS)
    def _():
        out_ref[...] = l_ref[jnp.minimum(me, PANELS - 1)].astype(F32)

    @pl.when(me >= PANELS)
    def _():
        rows = jnp.concatenate([l_ref[k] for k in range(PANELS)], axis=1)
        out_ref[...] = front_ref[...] - jnp.dot(rows, w_ref[...], preferred_element_type=F32)

        def add(n, carry):
            g = list_ref[n]
            for i in range(8):
                block = maps_ref[g, i] - s * SPAN

                @pl.when((block >= 0) & (block < SPAN))
                def _():
                    at = pl.ds(pl.multiple_of(block * W, W), W)
                    out_ref[at, :] += held[g, PACK + i * W : PACK + (i + 1) * W, :].astype(F32)

            return carry

        lax.fori_loop(0, list_ref[groups], add, 0)

        @pl.when(lax.div(me, SPAN) == s)
        def _():
            at = pl.ds(pl.multiple_of(lax.rem(me, SPAN) * W, W), W)
            row = lax.broadcasted_iota(jnp.int32, (W, W), 0)
            col = lax.broadcasted_iota(jnp.int32, (W, W), 1)
            out_ref[at, :] += jnp.where(row == col, flag_ref[...].astype(F32), 0.0)

        @pl.when(s == 0)
        def _():
            out_ref[:LEAD, :] = jnp.zeros((LEAD, W), F32)


def update(me, maps, front, all_l, w, parts, flags):
    order = front.shape[0]
    groups = parts.shape[0]
    return pl.pallas_call(
        update_kernel,
        out_shape=jax.ShapeDtypeStruct((order, W), F32),
        grid=(order // CHUNK,),
        in_specs=[
            pl.BlockSpec(memory_space=pltpu.SMEM),
            pl.BlockSpec(memory_space=pltpu.SMEM),
            pl.BlockSpec((CHUNK, W), lambda s: (s, 0)),
            pl.BlockSpec((PANELS, CHUNK, W), lambda s: (0, s, 0)),
            pl.BlockSpec((LEAD, W), lambda s: (0, 0)),
            pl.BlockSpec(memory_space=pl.ANY),
            pl.BlockSpec((1, W), lambda s: (0, 0)),
        ],
        out_specs=pl.BlockSpec((CHUNK, W), lambda s: (s, 0)),
        scratch_shapes=[
            pltpu.SMEM((groups + 1,), jnp.int32),
            pltpu.VMEM(parts.shape, BF16),
            pltpu.SemaphoreType.DMA((groups,)),
        ],
        name="update",
    )(me, maps, front, all_l, w, parts, flags)


def on_device(front, contributions, block_map, pivot_flags):
    me = lax.axis_index(("grp", "col"))
    which = me.reshape(1)
    order = front.shape[0]
    flags = pivot_flags.reshape(1, W)
    entries = jnp.broadcast_to(block_map.reshape(-1, 1).astype(BF16), (block_map.shape[1], W))
    packed = jnp.concatenate(
        [entries, jnp.zeros((PACK - entries.shape[0], W), BF16), contributions[0].astype(BF16)], axis=0
    )
    at = jnp.arange(LEAD, dtype=jnp.int32)[:, None] == me * W + jnp.arange(W, dtype=jnp.int32)[None, :]
    own = front[:LEAD] + jnp.where(at, flags.astype(F32), 0.0)
    cg, own, lead = exchange(packed, own)
    own_l, own_w = factor(which, lead, own)
    all_l = gather(own_l).reshape(PANELS, order, W)
    parts = cg.reshape(16, packed.shape[0], W)
    maps = parts[:, : block_map.shape[1], 0].astype(jnp.int32)
    return update(which, maps, front, all_l, own_w, parts, flags)


def solution(mesh):
    return jax.shard_map(
        on_device,
        mesh=mesh,
        in_specs=(
            P(None, ("grp", "col")),
            P("grp", None, "col"),
            P("grp", None),
            P(("grp", "col")),
        ),
        out_specs=P(None, ("grp", "col")),
        check_vma=False,
    )
```

```python
import jax
import jax.numpy as jnp
from jax import lax
from jax.experimental import pallas as pl
from jax.experimental.pallas import tpu as pltpu
from jax.sharding import PartitionSpec as P

PANELS = 4
W = 128
LEAD = PANELS * W
PACK = 16
CHILD = 1024
ROWS = PACK + CHILD
MESH = pl.DeviceIdType.MESH
FULL = pl.ds(0, 4)
F32 = jnp.float32
BF16 = jnp.bfloat16


def ldl_inverse(m_ref, d_ref, ticks):
    lane = lax.broadcasted_iota(jnp.int32, (8, W), 1)
    sub = lax.broadcasted_iota(jnp.int32, (8, W), 0)
    for g in range(W // 8):
        c0 = 8 * g
        rest = W - c0 - 8
        top = m_ref[c0 : c0 + 8, :]
        ctop = [jnp.broadcast_to(top[:, c0 + j : c0 + j + 1], (8, W)) for j in range(8)]
        if rest:
            low = m_ref[c0 + 8 :, :]
            clow = [jnp.broadcast_to(low[:, c0 + j : c0 + j + 1], (rest, W)) for j in range(8)]
        inside = (lane >= c0) & (lane < c0 + 8)
        rows = jnp.where(inside, (lane == sub + c0).astype(F32), top)
        dvec = jnp.zeros((8, W), F32)
        llow = []
        for j in range(8):
            piv = ctop[j][j : j + 1, :]
            rec = 1.0 / piv
            dvec = jnp.where(sub == j, piv, dvec)
            lt = jnp.where(sub > j, ctop[j] * rec, 0.0)
            ups = [ctop[jj][j : j + 1, :] for jj in range(j + 1, 8)]
            for jj, up in zip(range(j + 1, 8), ups):
                ctop[jj] = ctop[jj] - lt * up
            rows = rows - lt * rows[j : j + 1, :]
            if rest:
                ll = clow[j] * rec
                for jj, up in zip(range(j + 1, 8), ups):
                    clow[jj] = clow[jj] - ll * up
                llow.append(ll)
        m_ref[c0 : c0 + 8, :] = rows
        d_ref[c0 : c0 + 8, :] = dvec
        if rest:
            lanes = lax.broadcasted_iota(jnp.int32, (rest, W), 1)
            acc = jnp.where((lanes >= c0) & (lanes < c0 + 8), 0.0, low)
            for j in range(8):
                acc = acc - llow[j] * rows[j : j + 1, :]
            m_ref[c0 + 8 :, :] = acc
        for work in ticks.get(g, ()):
            work()


class Place:
    def __init__(self):
        self.g = lax.axis_index("grp")
        self.c = lax.axis_index("col")
        self.at = {"x": lax.rem(self.g, 4), "y": lax.div(self.g, 4), "z": lax.div(self.c, 2)}
        self.core = lax.rem(self.c, 2)
        self.partner = (self.g, self.at["z"] * 2 + 1 - self.core)

    def near(self, dim, delta):
        to = dict(self.at)
        to[dim] = lax.rem(self.at[dim] + delta + 4, 4)
        return (to["y"] * 4 + to["x"], to["z"] * 2 + self.core)

    def greet(self):
        barrier = pltpu.get_barrier_semaphore()
        peers = [self.near(d, s) for d in "xyz" for s in (1, -1)] + [self.partner]
        for peer in peers:
            pl.semaphore_signal(barrier, inc=1, device_id=peer, device_id_type=MESH)
        pl.semaphore_wait(barrier, len(peers))


class Wires:
    def __init__(self, send, recv, count):
        self.send, self.recv, self.count, self.used = send, recv, count, 0

    def copy(self, ref, device):
        n = self.used
        self.used += 1
        assert n < self.count
        return pltpu.make_async_remote_copy(
            src_ref=ref,
            dst_ref=ref,
            send_sem=self.send.at[n],
            recv_sem=self.recv.at[n],
            device_id=device,
            device_id_type=MESH,
        )


def gather_stream(place, wires, view, order, rows, middle, across):
    lo, hi = pl.ds(rows[0], middle - rows[0]), pl.ds(middle, rows[1] - middle)
    every = pl.ds(rows[0], rows[1] - rows[0])
    sent = []
    d2d = []

    def launch(copy, to=None):
        copy.start()
        sent.append(copy)
        if to is not None:
            to.append(copy)
        return copy

    for phase, dim in enumerate(order):
        last = across and phase == len(order) - 1

        def unit(v, r, dim=dim, phase=phase):
            where = {d: (FULL if d in order[:phase] else place.at[d]) for d in order}
            where[dim] = v
            return view(where, r)

        mine = place.at[dim]
        before, after, far = (lax.rem(mine + n, 4) for n in (3, 1, 2))
        right, left = place.near(dim, 1), place.near(dim, -1)
        to_right = launch(wires.copy(unit(mine, every), right))
        to_left = launch(wires.copy(unit(mine, every), left))
        if last:
            launch(wires.copy(unit(mine, every), place.partner), d2d)
        yield
        to_right.wait_recv()
        on_right = launch(wires.copy(unit(before, lo), right))
        if last:
            launch(wires.copy(unit(before, every), place.partner), d2d)
        to_left.wait_recv()
        on_left = launch(wires.copy(unit(after, hi), left))
        if last:
            launch(wires.copy(unit(after, every), place.partner), d2d)
        yield
        on_right.wait_recv()
        on_left.wait_recv()
        if last:
            launch(wires.copy(unit(far, every), place.partner), d2d)
    yield
    for copy in d2d:
        copy.wait_recv()
    yield
    for copy in sent:
        copy.wait_send()


def ring_bcast(on, r, wires, whole, lo, hi, right, left, partner=None, other=None):
    to_right, to_left = wires.copy(whole, right), wires.copy(whole, left)
    on_right, on_left = wires.copy(lo, right), wires.copy(hi, left)
    across = wires.copy(whole, partner) if partner is not None else None

    @pl.when(on & (r == 0))
    def _():
        to_right.start()
        to_left.start()
        if across is not None:
            across.start()

    yield

    @pl.when(on & (r == 1))
    def _():
        to_right.wait_recv()
        on_right.start()
        if across is not None:
            across.start()

    @pl.when(on & (r == 3))
    def _():
        to_left.wait_recv()
        on_left.start()
        if across is not None:
            across.start()

    yield

    @pl.when(on & (r == 2))
    def _():
        on_right.wait_recv()
        on_left.wait_recv()
        if across is not None:
            across.start()

    if across is not None:
        yield

        @pl.when(other)
        def _():
            across.wait_recv()

        yield

        @pl.when(on)
        def _():
            across.wait_send()

    @pl.when(on & (r == 0))
    def _():
        to_right.wait_send()
        to_left.wait_send()

    @pl.when(on & (r == 1))
    def _():
        on_right.wait_send()

    @pl.when(on & (r == 3))
    def _():
        on_left.wait_send()


class Round:
    def __init__(self, streams):
        self.streams = list(streams)

    def __call__(self):
        for s in self.streams:
            next(s, None)


TILES = ((4, 2, 2), (3, 3, 2), (4, 2, 2), (3, 2, 3))
ORDERS = ("xyz", "yzx", "zxy")
WIRES = 5 * 10 + 8 * 8 + 8 * 4 + 8 * 4 + 16 * 12
SLOTS = (2, 5, 8, 11, 14)


def panels_kernel(
    head_ref,
    child_ref,
    map_ref,
    flag_ref,
    all_ref,
    cg_ref,
    w_ref,
    maps_ref,
    own_ref,
    flead_ref,
    lead_ref,
    q_ref,
    coef_ref,
    m_ref,
    d_ref,
    rhs_ref,
    send_sem,
    recv_sem,
):
    place = Place()
    wires = Wires(send_sem, recv_sem, WIRES)
    x, y, z = place.at["x"], place.at["y"], place.at["z"]
    me = place.g * 8 + place.c
    low = place.c < PANELS
    row = lax.broadcasted_iota(jnp.int32, (W, W), 0)
    col = lax.broadcasted_iota(jnp.int32, (W, W), 1)

    entry = lax.broadcasted_iota(jnp.int32, (PACK, W), 0)
    packed = jnp.zeros((PACK, W), F32)
    for i in range(8):
        packed = jnp.where(entry == i, map_ref[0, i].astype(F32), packed)
    cg_ref[y, x, 0:PACK, :] = packed.astype(BF16)
    cg_ref[y, x, PACK:ROWS, :] = child_ref[0].astype(BF16)
    own_ref[...] = head_ref[...]
    for k in range(PANELS):

        @pl.when(me == k)
        def _():
            at = pl.ds(k * W, W)
            own_ref[at, :] += jnp.where(row == col, flag_ref[...].astype(F32), 0.0)

    @pl.when((place.g == 0) & low)
    def _():
        flead_ref[...] = own_ref[...]

    place.greet()

    def child_view(where, rows):
        return cg_ref.at[where["y"], where["x"], rows, :]

    def child_stream(r0, r1, order):
        middle = r0 + (r1 - r0 + 16) // 32 * 16
        return gather_stream(place, wires, child_view, order, (r0, r1), middle, False)

    def spread(j):
        first, second = ("x", "y") if j % 2 == 0 else ("y", "x")
        base = j * W
        half = W // 2
        refs = [flead_ref.at[pl.ds(at, size)] for at, size in ((base, W), (base, half), (base + half, half))]
        for dim, on in ((first, low & (place.at[second] == 0)), (second, low)):
            yield from ring_bcast(on, place.at[dim], wires, *refs, place.near(dim, 1), place.near(dim, -1))

    def lead_unit(l, k):
        on = place.core == l % 2
        r = lax.rem(z - l // 2 + 4, 4)
        half = W // 2
        refs = [lead_ref.at[l, k], lead_ref.at[l, k, pl.ds(0, half)], lead_ref.at[l, k, pl.ds(half, half)]]
        return ring_bcast(
            on, r, wires, *refs, place.near("z", 1), place.near("z", -1), place.partner, place.core != l % 2
        )

    def panel_stream(k, p):
        def view(where, rows):
            return all_ref.at[k, where["y"], where["x"], where["z"], place.core, rows, :]

        r0 = 16 * sum(TILES[k][:p])
        n = TILES[k][p]
        half = (n // 2 if (k + p) % 2 else (n + 1) // 2) * 16
        return gather_stream(place, wires, view, ORDERS[p], (r0, r0 + 16 * n), r0 + half, True)

    def first_row(s):
        return PACK + s * W if s else 0

    a = [
        Round(
            [
                child_stream(first_row(s), PACK + s * W + 64, "xy"),
                child_stream(PACK + s * W + 64, PACK + s * W + W, "yx"),
                spread(s),
            ]
        )
        for s in range(PANELS)
    ]
    far = PACK + LEAD
    b = [
        Round([child_stream(far + n * W, far + (n + 1) * W, "xy" if n % 2 == 0 else "yx") for n in (m, m + 1)])
        for m in (0, 2)
    ]
    lead = [Round([lead_unit(l, k) for l in range(k, PANELS)]) for k in range(PANELS)]
    g = [Round([panel_stream(k, p) for p in range(3)]) for k in range(PANELS)]

    def assemble(k):
        at = pl.ds(k * W, W)
        acc_own, acc_lead = own_ref[at, :], flead_ref[at, :]
        for child in range(16):
            cy, cx = child // 4, child % 4
            names = cg_ref[cy, cx, 0:PACK, :].astype(F32)
            target = jnp.sum(jnp.where(entry == place.c, names, 0.0), axis=0, keepdims=True)
            here = names[k : k + 1, :] == float(k)
            mine = jnp.where((target == me.astype(F32)) & here, 1.0, 0.0)
            first = jnp.where((target == place.c.astype(F32)) & here, 1.0, 0.0)
            block = cg_ref[cy, cx, PACK + k * W : PACK + (k + 1) * W, :].astype(F32)
            acc_own = acc_own + block * mine
            acc_lead = acc_lead + block * first
            if k == 0:
                diagonal = lax.broadcasted_iota(jnp.int32, (PACK, W), 1) == entry
                line = jnp.sum(jnp.where(diagonal, names, 0.0), axis=0, keepdims=True)
                maps_ref[child : child + 1, :] = line.astype(jnp.int32)
        own_ref[at, :] = acc_own
        for l in range(k, PANELS):

            @pl.when(place.c == l)
            def _():
                lead_ref[l, k] = acc_lead

    def panel(k, plan):
        width = PANELS - 1 - k
        at = pl.ds(k * W, W)
        base = jnp.concatenate([lead_ref[l, k] for l in range(k, PANELS)] + [own_ref[at, :]], axis=1)
        if k:
            base = base - jnp.dot(
                coef_ref[k * W : (k + 1) * W, : k * W], q_ref[: k * W, k * W :], preferred_element_type=F32
            )
        diag = base[:, :W]
        diag = 0.5 * (diag + diag.T)
        m_ref[...] = diag
        rhs_ref[:, :W] = jnp.where(me == k, diag, base[:, (width + 1) * W :])
        if width:
            rhs_ref[:, W : W + width * W] = base[:, W : W + width * W]
        ldl_inverse(m_ref, d_ref, dict(zip(SLOTS, plan)))
        d = d_ref[...]
        minv = jnp.where(col <= row, m_ref[...], 0.0) / d
        piv = d.astype(BF16).astype(F32)
        rhs = rhs_ref[:, : W + width * W]
        q = jnp.dot(minv, rhs, precision=lax.Precision.HIGHEST, preferred_element_type=F32)
        own = jnp.where((me > k) | ((me == k) & (col >= row)), q[:, :W], 0.0).astype(BF16).astype(F32)
        all_ref[k, y, x, z, place.core] = own.T.astype(BF16)
        g[k]()
        w_ref[k * W : (k + 1) * W, :] = (own * piv).astype(BF16)
        q_ref[k * W : (k + 1) * W, LEAD:] = own.astype(BF16)
        for i in range(width):
            l = k + 1 + i
            part = q[:, (1 + i) * W : (2 + i) * W].astype(BF16)
            q_ref[k * W : (k + 1) * W, l * W : (l + 1) * W] = part
            coef_ref[l * W : (l + 1) * W, k * W : (k + 1) * W] = (
                (part.astype(F32) * piv).astype(BF16).astype(F32).T.astype(BF16)
            )

    def join(k):
        return lambda: assemble(k)

    for s in range(PANELS):
        a[s]()
    for s in range(PANELS):
        a[s]()
    for work in (a[0], a[0], a[1], a[0], join(0), lead[0], a[1], lead[0], a[2], a[1], lead[0], join(1), lead[0]):
        work()
    lead[1]()
    a[2]()
    panel(
        0,
        (
            (lead[1], a[3]),
            (lead[1], a[2]),
            (lead[1], join(2), lead[2]),
            (a[3], b[0]),
            (lead[2], a[3]),
        ),
    )
    panel(
        1,
        (
            (g[0], lead[2]),
            (join(3), lead[3], lead[2], b[0]),
            (g[0], lead[3]),
            (b[0], g[0]),
            (lead[3],),
        ),
    )
    panel(
        2,
        (
            (g[0], lead[3], g[1]),
            (b[0], g[1]),
            (g[0],),
            (g[1], b[0], b[1]),
            (g[0],),
        ),
    )
    panel(
        3,
        (
            (g[2], g[1], b[1]),
            (g[2], g[0]),
            (g[1], b[1]),
            (g[2],),
            (g[1], b[1]),
        ),
    )
    for work in (g[3], g[2], g[3], g[1], g[3], g[2], b[1], g[3], g[2], g[3], g[2], g[3], g[3]):
        work()
    for group in a + b + lead + g:
        for stream in group.streams:
            for _ in stream:
                pass
    assert wires.used == WIRES


def panels(head, contributions, block_map, flags):
    vmem = pl.BlockSpec(memory_space=pltpu.VMEM)
    return pl.pallas_call(
        panels_kernel,
        out_shape=(
            pltpu.VMEM((PANELS, 4, 4, 4, 2, W, W), BF16),
            pltpu.VMEM((4, 4, ROWS, W), BF16),
            pltpu.VMEM((LEAD, W), BF16),
            jax.ShapeDtypeStruct((16, W), jnp.int32),
        ),
        in_specs=[vmem, vmem, pl.BlockSpec(memory_space=pltpu.SMEM), vmem],
        out_specs=(vmem, vmem, vmem, vmem),
        scratch_shapes=[
            pltpu.VMEM((LEAD, W), F32),
            pltpu.VMEM((LEAD, W), F32),
            pltpu.VMEM((PANELS, PANELS, W, W), F32),
            pltpu.VMEM((LEAD, LEAD + W), BF16),
            pltpu.VMEM((LEAD, LEAD), BF16),
            pltpu.VMEM((W, W), F32),
            pltpu.VMEM((W, W), F32),
            pltpu.VMEM((W, LEAD), F32),
            pltpu.SemaphoreType.DMA((WIRES,)),
            pltpu.SemaphoreType.DMA((WIRES,)),
        ],
        compiler_params=pltpu.CompilerParams(
            collective_id=0, has_side_effects=True, vmem_limit_bytes=VMEM_PANELS
        ),
        name="panels",
    )(head, contributions, block_map, flags)


VMEM_PANELS = 12 * 2**20
VMEM_UPDATE = 12 * 2**20
CHUNK = 2048
SPAN = CHUNK // W


def update_kernel(me_ref, maps_ref, front_ref, l_ref, w_ref, parts_ref, flag_ref, out_ref, list_ref):
    s = pl.program_id(0)
    me = me_ref[0]
    groups = parts_ref.shape[0]
    rows = pl.ds(pl.multiple_of(s * CHUNK, CHUNK), CHUNK)

    @pl.when(s == 0)
    def _():
        count = jnp.int32(0)
        for g in range(groups):
            mine = maps_ref[g, lax.rem(me, 8)] == me
            list_ref[count] = g
            count = count + mine.astype(jnp.int32)
        list_ref[groups] = count

    @pl.when(me < PANELS)
    def _():
        out_ref[...] = l_ref[jnp.minimum(me, PANELS - 1), rows, :].astype(F32)

    @pl.when(me >= PANELS)
    def _():
        left = jnp.concatenate([l_ref[k, rows, :] for k in range(PANELS)], axis=1)
        out_ref[...] = front_ref[rows, :] - jnp.dot(left, w_ref[...], preferred_element_type=F32)

        def add(n, carry):
            g = list_ref[n]
            for i in range(8):
                block = maps_ref[g, i] - s * SPAN

                @pl.when((block >= 0) & (block < SPAN))
                def _():
                    at = pl.ds(pl.multiple_of(block * W, W), W)
                    out_ref[at, :] += parts_ref[g, PACK + i * W : PACK + (i + 1) * W, :].astype(F32)

            return carry

        lax.fori_loop(0, list_ref[groups], add, 0)

        @pl.when(lax.div(me, SPAN) == s)
        def _():
            at = pl.ds(pl.multiple_of(lax.rem(me, SPAN) * W, W), W)
            row = lax.broadcasted_iota(jnp.int32, (W, W), 0)
            col = lax.broadcasted_iota(jnp.int32, (W, W), 1)
            out_ref[at, :] += jnp.where(row == col, flag_ref[...].astype(F32), 0.0)

        @pl.when(s == 0)
        def _():
            out_ref[:LEAD, :] = jnp.zeros((LEAD, W), F32)


def update(me, maps, front, all_l, w, parts, flags):
    order = front.shape[0]
    vmem = pl.BlockSpec(memory_space=pltpu.VMEM)
    smem = pl.BlockSpec(memory_space=pltpu.SMEM)
    return pl.pallas_call(
        update_kernel,
        out_shape=jax.ShapeDtypeStruct((order, W), F32),
        grid=(order // CHUNK,),
        in_specs=[smem, smem, vmem, vmem, vmem, vmem, vmem],
        out_specs=pl.BlockSpec((CHUNK, W), lambda s: (s, 0)),
        scratch_shapes=[pltpu.SMEM((parts.shape[0] + 1,), jnp.int32)],
        compiler_params=pltpu.CompilerParams(vmem_limit_bytes=VMEM_UPDATE),
        name="update",
    )(me, maps, front, all_l, w, parts, flags)


def on_device(front, contributions, block_map, pivot_flags):
    which = lax.axis_index(("grp", "col")).reshape(1)
    flags = pivot_flags.reshape(1, W)
    all_l, parts, w, maps = panels(front[:LEAD], contributions, block_map, flags)
    all_l = all_l.reshape(PANELS, front.shape[0], W)
    return update(which, maps, front, all_l, w, parts.reshape(16, ROWS, W), flags)


def solution(mesh):
    return jax.shard_map(
        on_device,
        mesh=mesh,
        in_specs=(
            P(None, ("grp", "col")),
            P("grp", None, "col"),
            P("grp", None),
            P(("grp", "col")),
        ),
        out_specs=P(None, ("grp", "col")),
        check_vma=False,
    )
```

```python
import jax
import jax.numpy as jnp
from jax import lax
from jax.experimental import pallas as pl
from jax.experimental.pallas import tpu as pltpu
from jax.sharding import PartitionSpec as P

PANELS = 4
W = 128
LEAD = PANELS * W
PACK = 16
CHILD = 1024
ROWS = PACK + CHILD
MESH = pl.DeviceIdType.MESH
FULL = pl.ds(0, 4)
F32 = jnp.float32
BF16 = jnp.bfloat16


def ldl_inverse(m_ref, d_ref, ticks):
    lane = lax.broadcasted_iota(jnp.int32, (8, W), 1)
    sub = lax.broadcasted_iota(jnp.int32, (8, W), 0)
    for g in range(W // 8):
        c0 = 8 * g
        rest = W - c0 - 8
        top = m_ref[c0 : c0 + 8, :]
        ctop = [jnp.broadcast_to(top[:, c0 + j : c0 + j + 1], (8, W)) for j in range(8)]
        if rest:
            low = m_ref[c0 + 8 :, :]
            clow = [jnp.broadcast_to(low[:, c0 + j : c0 + j + 1], (rest, W)) for j in range(8)]
        inside = (lane >= c0) & (lane < c0 + 8)
        rows = jnp.where(inside, (lane == sub + c0).astype(F32), top)
        dvec = jnp.zeros((8, W), F32)
        llow = []
        for j in range(8):
            piv = ctop[j][j : j + 1, :]
            rec = 1.0 / piv
            dvec = jnp.where(sub == j, piv, dvec)
            lt = jnp.where(sub > j, ctop[j] * rec, 0.0)
            ups = [ctop[jj][j : j + 1, :] for jj in range(j + 1, 8)]
            for jj, up in zip(range(j + 1, 8), ups):
                ctop[jj] = ctop[jj] - lt * up
            rows = rows - lt * rows[j : j + 1, :]
            if rest:
                ll = clow[j] * rec
                for jj, up in zip(range(j + 1, 8), ups):
                    clow[jj] = clow[jj] - ll * up
                llow.append(ll)
        m_ref[c0 : c0 + 8, :] = rows
        d_ref[c0 : c0 + 8, :] = dvec
        if rest:
            lanes = lax.broadcasted_iota(jnp.int32, (rest, W), 1)
            acc = jnp.where((lanes >= c0) & (lanes < c0 + 8), 0.0, low)
            for j in range(8):
                acc = acc - llow[j] * rows[j : j + 1, :]
            m_ref[c0 + 8 :, :] = acc
        for work in ticks.get(g, ()):
            work()


class Place:
    def __init__(self):
        self.g = lax.axis_index("grp")
        self.c = lax.axis_index("col")
        self.at = {"x": lax.rem(self.g, 4), "y": lax.div(self.g, 4), "z": lax.div(self.c, 2)}
        self.core = lax.rem(self.c, 2)
        self.partner = (self.g, self.at["z"] * 2 + 1 - self.core)

    def near(self, dim, delta):
        to = dict(self.at)
        to[dim] = lax.rem(self.at[dim] + delta + 4, 4)
        return (to["y"] * 4 + to["x"], to["z"] * 2 + self.core)

    def greet(self):
        barrier = pltpu.get_barrier_semaphore()
        peers = [self.near(d, s) for d in "xyz" for s in (1, 2, 3)] + [self.partner]
        for peer in peers:
            pl.semaphore_signal(barrier, inc=1, device_id=peer, device_id_type=MESH)
        pl.semaphore_wait(barrier, len(peers))


class Wires:
    def __init__(self, send, recv, count):
        self.send, self.recv, self.count, self.used = send, recv, count, 0

    def copy(self, ref, device):
        n = self.used
        self.used += 1
        assert n < self.count
        return pltpu.make_async_remote_copy(
            src_ref=ref,
            dst_ref=ref,
            send_sem=self.send.at[n],
            recv_sem=self.recv.at[n],
            device_id=device,
            device_id_type=MESH,
        )


def gather_stream(place, wires, view, order, rows, middle, across, direct):
    lo, hi = pl.ds(rows[0], middle - rows[0]), pl.ds(middle, rows[1] - middle)
    every = pl.ds(rows[0], rows[1] - rows[0])
    sent = []
    d2d = []

    def launch(copy, to=None):
        copy.start()
        sent.append(copy)
        if to is not None:
            to.append(copy)
        return copy

    for phase, dim in enumerate(order):
        last = across and phase == len(order) - 1

        def unit(v, r, dim=dim, phase=phase):
            where = {d: (FULL if d in order[:phase] else place.at[d]) for d in order}
            where[dim] = v
            return view(where, r)

        mine = place.at[dim]
        before, after, far = (lax.rem(mine + n, 4) for n in (3, 1, 2))
        right, left = place.near(dim, 1), place.near(dim, -1)
        to_right = launch(wires.copy(unit(mine, every), right))
        to_left = launch(wires.copy(unit(mine, every), left))
        if phase < direct:
            to_far = launch(wires.copy(unit(mine, every), place.near(dim, 2)))
            yield
            to_right.wait_recv()
            to_left.wait_recv()
            to_far.wait_recv()
            continue
        if last:
            launch(wires.copy(unit(mine, every), place.partner), d2d)
        yield
        to_right.wait_recv()
        on_right = launch(wires.copy(unit(before, lo), right))
        if last:
            launch(wires.copy(unit(before, every), place.partner), d2d)
        to_left.wait_recv()
        on_left = launch(wires.copy(unit(after, hi), left))
        if last:
            launch(wires.copy(unit(after, every), place.partner), d2d)
        yield
        on_right.wait_recv()
        on_left.wait_recv()
        if last:
            launch(wires.copy(unit(far, every), place.partner), d2d)
    yield
    for copy in d2d:
        copy.wait_recv()
    yield
    for copy in sent:
        copy.wait_send()


def straight_bcast(on, r, wires, whole, near, partner=None, other=None):
    legs = [wires.copy(whole, near(n)) for n in (1, 2, 3)]
    across = wires.copy(whole, partner) if partner is not None else None

    @pl.when(on & (r == 0))
    def _():
        for leg in (legs[1], legs[0], legs[2]):
            leg.start()
        if across is not None:
            across.start()

    yield
    for n in (1, 2, 3):

        @pl.when(on & (r == n))
        def _():
            legs[n - 1].wait_recv()
            if across is not None:
                across.start()

    if across is not None:
        yield

        @pl.when(other)
        def _():
            across.wait_recv()

        yield

        @pl.when(on)
        def _():
            across.wait_send()

    @pl.when(on & (r == 0))
    def _():
        for leg in legs:
            leg.wait_send()


def ring_bcast(on, r, wires, whole, lo, hi, right, left, partner=None, other=None):
    to_right, to_left = wires.copy(whole, right), wires.copy(whole, left)
    on_right, on_left = wires.copy(lo, right), wires.copy(hi, left)
    across = wires.copy(whole, partner) if partner is not None else None

    @pl.when(on & (r == 0))
    def _():
        to_right.start()
        to_left.start()
        if across is not None:
            across.start()

    yield

    @pl.when(on & (r == 1))
    def _():
        to_right.wait_recv()
        on_right.start()
        if across is not None:
            across.start()

    @pl.when(on & (r == 3))
    def _():
        to_left.wait_recv()
        on_left.start()
        if across is not None:
            across.start()

    yield

    @pl.when(on & (r == 2))
    def _():
        on_right.wait_recv()
        on_left.wait_recv()
        if across is not None:
            across.start()

    if across is not None:
        yield

        @pl.when(other)
        def _():
            across.wait_recv()

        yield

        @pl.when(on)
        def _():
            across.wait_send()

    @pl.when(on & (r == 0))
    def _():
        to_right.wait_send()
        to_left.wait_send()

    @pl.when(on & (r == 1))
    def _():
        on_right.wait_send()

    @pl.when(on & (r == 3))
    def _():
        on_left.wait_send()


class Round:
    def __init__(self, streams):
        self.streams = list(streams)

    def __call__(self):
        for s in self.streams:
            next(s, None)


TILES = ((3, 3, 2), (3, 2, 3), (2, 3, 3), (3, 3, 2))
ORDERS = ("xyz", "yzx", "zxy")
WIRES = 4 * 7 + 5 * 3 + 6 * 2 + 6 * 7 + 3 * 2 + 4 * 6 + 4 * 7 + 15 * 12
SLOTS = (5, 10, 15)


def panels_kernel(
    head_ref,
    child_ref,
    map_ref,
    flag_ref,
    all_ref,
    cg_ref,
    w_ref,
    maps_ref,
    own_ref,
    flead_ref,
    lead_ref,
    q_ref,
    coef_ref,
    m_ref,
    d_ref,
    rhs_ref,
    send_sem,
    recv_sem,
):
    place = Place()
    wires = Wires(send_sem, recv_sem, WIRES)
    x, y, z = place.at["x"], place.at["y"], place.at["z"]
    me = place.g * 8 + place.c
    low = place.c < PANELS
    row = lax.broadcasted_iota(jnp.int32, (W, W), 0)
    col = lax.broadcasted_iota(jnp.int32, (W, W), 1)

    entry = lax.broadcasted_iota(jnp.int32, (PACK, W), 0)
    packed = jnp.zeros((PACK, W), F32)
    for i in range(8):
        packed = jnp.where(entry == i, map_ref[0, i].astype(F32), packed)
    cg_ref[y, x, 0:PACK, :] = packed.astype(BF16)
    cg_ref[y, x, PACK:ROWS, :] = child_ref[0].astype(BF16)
    own_ref[...] = head_ref[...]
    for k in range(PANELS):

        @pl.when(me == k)
        def _():
            at = pl.ds(k * W, W)
            own_ref[at, :] += jnp.where(row == col, flag_ref[...].astype(F32), 0.0)

    @pl.when((place.g == 0) & low)
    def _():
        flead_ref[...] = own_ref[...]

    place.greet()

    def child_view(where, rows):
        return cg_ref.at[where["y"], where["x"], rows, :]

    def child_stream(r0, r1, order, direct=1):
        middle = r0 + (r1 - r0 + 16) // 32 * 16
        return gather_stream(place, wires, child_view, order, (r0, r1), middle, False, direct)

    def spread(j):
        first, second = ("x", "y") if j % 2 == 0 else ("y", "x")
        base = j * W
        half = W // 2
        refs = [flead_ref.at[pl.ds(at, size)] for at, size in ((base, W), (base, half), (base + half, half))]
        for dim, on in ((first, low & (place.at[second] == 0)), (second, low)):
            if j == 0:
                yield from straight_bcast(on, place.at[dim], wires, refs[0], lambda n, dim=dim: place.near(dim, n))
            else:
                yield from ring_bcast(on, place.at[dim], wires, *refs, place.near(dim, 1), place.near(dim, -1))

    def lead_unit(l, k):
        on = place.core == l % 2
        r = lax.rem(z - l // 2 + 4, 4)
        half = W // 2
        if k < 2:
            return straight_bcast(
                on, r, wires, lead_ref.at[l, k], lambda n: place.near("z", n), place.partner, place.core != l % 2
            )
        refs = [lead_ref.at[l, k], lead_ref.at[l, k, pl.ds(0, half)], lead_ref.at[l, k, pl.ds(half, half)]]
        return ring_bcast(
            on, r, wires, *refs, place.near("z", 1), place.near("z", -1), place.partner, place.core != l % 2
        )

    def panel_stream(k, p):
        def view(where, rows):
            return all_ref.at[k, where["y"], where["x"], where["z"], place.core, rows, :]

        r0 = 16 * sum(TILES[k][:p])
        n = TILES[k][p]
        half = (n // 2 if (k + p) % 2 else (n + 1) // 2) * 16
        return gather_stream(place, wires, view, ORDERS[p], (r0, r0 + 16 * n), r0 + half, True, 1)

    def first_row(s):
        return PACK + s * W if s else 0

    a = [
        Round(
            [
                child_stream(first_row(s), PACK + s * W + 64, "xy", 1 if s else 2),
                child_stream(PACK + s * W + 64, PACK + s * W + W, "yx", 1 if s else 2),
            ]
        )
        for s in range(PANELS)
    ]
    f = [Round([spread(s)]) for s in range(PANELS)]
    far = PACK + LEAD
    b = [
        Round([child_stream(far + n * W, far + (n + 1) * W, "xy" if n % 2 == 0 else "yx") for n in (m, m + 1)])
        for m in (0, 2)
    ]
    lead = [Round([lead_unit(l, k) for l in range(k, PANELS)]) for k in range(PANELS)]
    g = [Round([panel_stream(k, p) for p in range(3)]) for k in range(PANELS)]

    def assemble(k):
        at = pl.ds(k * W, W)
        acc_own, acc_lead = own_ref[at, :], flead_ref[at, :]
        for child in range(16):
            cy, cx = child // 4, child % 4
            names = cg_ref[cy, cx, 0:PACK, :].astype(F32)
            target = jnp.sum(jnp.where(entry == place.c, names, 0.0), axis=0, keepdims=True)
            here = names[k : k + 1, :] == float(k)
            mine = jnp.where((target == me.astype(F32)) & here, 1.0, 0.0)
            first = jnp.where((target == place.c.astype(F32)) & here, 1.0, 0.0)
            block = cg_ref[cy, cx, PACK + k * W : PACK + (k + 1) * W, :].astype(F32)
            acc_own = acc_own + block * mine
            acc_lead = acc_lead + block * first
            if k == 0:
                diagonal = lax.broadcasted_iota(jnp.int32, (PACK, W), 1) == entry
                line = jnp.sum(jnp.where(diagonal, names, 0.0), axis=0, keepdims=True)
                maps_ref[child : child + 1, :] = line.astype(jnp.int32)
        own_ref[at, :] = acc_own
        for l in range(k, PANELS):

            @pl.when(place.c == l)
            def _():
                lead_ref[l, k] = acc_lead

    def panel(k, plan):
        width = PANELS - 1 - k
        at = pl.ds(k * W, W)
        base = jnp.concatenate([lead_ref[l, k] for l in range(k, PANELS)] + [own_ref[at, :]], axis=1)
        if k:
            base = base - jnp.dot(
                coef_ref[k * W : (k + 1) * W, : k * W], q_ref[: k * W, k * W :], preferred_element_type=F32
            )
        diag = base[:, :W]
        diag = 0.5 * (diag + diag.T)
        m_ref[...] = diag
        rhs_ref[:, :W] = jnp.where(me == k, diag, base[:, (width + 1) * W :])
        if width:
            rhs_ref[:, W : W + width * W] = base[:, W : W + width * W]
        ldl_inverse(m_ref, d_ref, dict(zip(SLOTS, plan)))
        d = d_ref[...]
        minv = jnp.where(col <= row, m_ref[...], 0.0) / d
        piv = d.astype(BF16).astype(F32)
        rhs = rhs_ref[:, : W + width * W]
        q = jnp.dot(minv, rhs, precision=lax.Precision.HIGHEST, preferred_element_type=F32)
        own = jnp.where((me > k) | ((me == k) & (col >= row)), q[:, :W], 0.0).astype(BF16).astype(F32)
        all_ref[k, y, x, z, place.core] = own.T.astype(BF16)
        g[k]()
        w_ref[k * W : (k + 1) * W, :] = (own * piv).astype(BF16)
        q_ref[k * W : (k + 1) * W, LEAD:] = own.astype(BF16)
        for i in range(width):
            l = k + 1 + i
            part = q[:, (1 + i) * W : (2 + i) * W].astype(BF16)
            q_ref[k * W : (k + 1) * W, l * W : (l + 1) * W] = part
            coef_ref[l * W : (l + 1) * W, k * W : (k + 1) * W] = (
                (part.astype(F32) * piv).astype(BF16).astype(F32).T.astype(BF16)
            )

    def run(*rounds):
        for work in rounds:
            work()

    late = (1, 2, 3)

    def begin(k):
        assemble(k)
        lead[k]()

    run(a[0], f[0], *[a[k] for k in late], *[f[k] for k in late])
    run(a[0], f[0], *[f[k] for k in late], *[a[k] for k in late])
    run(a[0], f[0])
    begin(0)
    run(*[f[k] for k in late], b[0], b[1], lead[0], *[a[k] for k in late], lead[0])
    panel(
        0,
        (
            (*[f[k] for k in late], *[a[k] for k in late], b[0], b[1]),
            (*[f[k] for k in late], lambda: [begin(k) for k in late]),
            (lead[1],),
        ),
    )
    run(lead[1], lead[2], lead[3], g[0])
    panel(1, ((b[0], b[1]), (g[0], lead[2], lead[3]), (lead[2], lead[3])))
    run(g[0])
    panel(2, ((g[1],), (b[0], b[1]), (g[1],)))
    run(g[0])
    panel(3, ((g[1],), (g[2],), (g[0],)))
    run(g[2], g[1], g[3], g[2], g[1], g[3], g[0], g[2], g[3], g[1], g[2], g[3], g[3], g[2], g[3])
    for group in a + f + b + lead + g:
        for stream in group.streams:
            for _ in stream:
                pass
    assert wires.used == WIRES


def panels(head, contributions, block_map, flags):
    vmem = pl.BlockSpec(memory_space=pltpu.VMEM)
    return pl.pallas_call(
        panels_kernel,
        out_shape=(
            pltpu.VMEM((PANELS, 4, 4, 4, 2, W, W), BF16),
            pltpu.VMEM((4, 4, ROWS, W), BF16),
            pltpu.VMEM((LEAD, W), BF16),
            jax.ShapeDtypeStruct((16, W), jnp.int32),
        ),
        in_specs=[vmem, vmem, pl.BlockSpec(memory_space=pltpu.SMEM), vmem],
        out_specs=(vmem, vmem, vmem, vmem),
        scratch_shapes=[
            pltpu.VMEM((LEAD, W), F32),
            pltpu.VMEM((LEAD, W), F32),
            pltpu.VMEM((PANELS, PANELS, W, W), F32),
            pltpu.VMEM((LEAD, LEAD + W), BF16),
            pltpu.VMEM((LEAD, LEAD), BF16),
            pltpu.VMEM((W, W), F32),
            pltpu.VMEM((W, W), F32),
            pltpu.VMEM((W, LEAD), F32),
            pltpu.SemaphoreType.DMA((WIRES,)),
            pltpu.SemaphoreType.DMA((WIRES,)),
        ],
        compiler_params=pltpu.CompilerParams(
            collective_id=0, has_side_effects=True, vmem_limit_bytes=VMEM_PANELS
        ),
        cost_estimate=pl.CostEstimate(flops=2 * 10**10, bytes_accessed=3 * 2**20, transcendentals=0),
        name="panels",
    )(head, contributions, block_map, flags)


VMEM_PANELS = 12 * 2**20
VMEM_UPDATE = 12 * 2**20
CHUNK = 2048
SPAN = CHUNK // W


def update_kernel(me_ref, maps_ref, front_ref, l_ref, w_ref, parts_ref, flag_ref, out_ref, list_ref):
    s = pl.program_id(0)
    me = me_ref[0]
    groups = parts_ref.shape[0]
    rows = pl.ds(pl.multiple_of(s * CHUNK, CHUNK), CHUNK)

    @pl.when(s == 0)
    def _():
        count = jnp.int32(0)
        for g in range(groups):
            mine = maps_ref[g, lax.rem(me, 8)] == me
            list_ref[count] = g
            count = count + mine.astype(jnp.int32)
        list_ref[groups] = count

    @pl.when(me < PANELS)
    def _():
        out_ref[...] = l_ref[jnp.minimum(me, PANELS - 1), rows, :].astype(F32)

    @pl.when(me >= PANELS)
    def _():
        left = jnp.concatenate([l_ref[k, rows, :] for k in range(PANELS)], axis=1)
        out_ref[...] = front_ref[rows, :] - jnp.dot(left, w_ref[...], preferred_element_type=F32)

        def add(n, carry):
            g = list_ref[n]
            for i in range(8):
                block = maps_ref[g, i] - s * SPAN

                @pl.when((block >= 0) & (block < SPAN))
                def _():
                    at = pl.ds(pl.multiple_of(block * W, W), W)
                    out_ref[at, :] += parts_ref[g, PACK + i * W : PACK + (i + 1) * W, :].astype(F32)

            return carry

        lax.fori_loop(0, list_ref[groups], add, 0)

        @pl.when(lax.div(me, SPAN) == s)
        def _():
            at = pl.ds(pl.multiple_of(lax.rem(me, SPAN) * W, W), W)
            row = lax.broadcasted_iota(jnp.int32, (W, W), 0)
            col = lax.broadcasted_iota(jnp.int32, (W, W), 1)
            out_ref[at, :] += jnp.where(row == col, flag_ref[...].astype(F32), 0.0)

        @pl.when(s == 0)
        def _():
            out_ref[:LEAD, :] = jnp.zeros((LEAD, W), F32)


def update(me, maps, front, all_l, w, parts, flags):
    order = front.shape[0]
    vmem = pl.BlockSpec(memory_space=pltpu.VMEM)
    smem = pl.BlockSpec(memory_space=pltpu.SMEM)
    return pl.pallas_call(
        update_kernel,
        out_shape=jax.ShapeDtypeStruct((order, W), F32),
        grid=(order // CHUNK,),
        in_specs=[smem, smem, vmem, vmem, vmem, vmem, vmem],
        out_specs=pl.BlockSpec((CHUNK, W), lambda s: (s, 0)),
        scratch_shapes=[pltpu.SMEM((parts.shape[0] + 1,), jnp.int32)],
        compiler_params=pltpu.CompilerParams(vmem_limit_bytes=VMEM_UPDATE),
        name="update",
    )(me, maps, front, all_l, w, parts, flags)


def on_device(front, contributions, block_map, pivot_flags):
    which = lax.axis_index(("grp", "col")).reshape(1)
    flags = pivot_flags.reshape(1, W)
    all_l, parts, w, maps = panels(front[:LEAD], contributions, block_map, flags)
    all_l = all_l.reshape(PANELS, front.shape[0], W)
    return update(which, maps, front, all_l, w, parts.reshape(16, ROWS, W), flags)


def solution(mesh):
    return jax.shard_map(
        on_device,
        mesh=mesh,
        in_specs=(
            P(None, ("grp", "col")),
            P("grp", None, "col"),
            P("grp", None),
            P(("grp", "col")),
        ),
        out_specs=P(None, ("grp", "col")),
        check_vma=False,
    )
```

```python
import jax
import jax.numpy as jnp
from jax import lax
from jax.experimental import pallas as pl
from jax.experimental.pallas import tpu as pltpu
from jax.sharding import PartitionSpec as P

PANELS = 4
W = 128
LEAD = PANELS * W
PACK = 16
CHILD = 1024
ROWS = PACK + CHILD
MESH = pl.DeviceIdType.MESH
FULL = pl.ds(0, 4)
F32 = jnp.float32
BF16 = jnp.bfloat16


def ldl_inverse(m_ref, d_ref, ticks):
    lane = lax.broadcasted_iota(jnp.int32, (8, W), 1)
    sub = lax.broadcasted_iota(jnp.int32, (8, W), 0)
    for g in range(W // 8):
        c0 = 8 * g
        rest = W - c0 - 8
        top = m_ref[c0 : c0 + 8, :]
        ctop = [jnp.broadcast_to(top[:, c0 + j : c0 + j + 1], (8, W)) for j in range(8)]
        if rest:
            low = m_ref[c0 + 8 :, :]
            clow = [jnp.broadcast_to(low[:, c0 + j : c0 + j + 1], (rest, W)) for j in range(8)]
        inside = (lane >= c0) & (lane < c0 + 8)
        rows = jnp.where(inside, (lane == sub + c0).astype(F32), top)
        dvec = jnp.zeros((8, W), F32)
        llow = []
        for j in range(8):
            piv = ctop[j][j : j + 1, :]
            rec = 1.0 / piv
            dvec = jnp.where(sub == j, piv, dvec)
            lt = jnp.where(sub > j, ctop[j] * rec, 0.0)
            ups = [ctop[jj][j : j + 1, :] for jj in range(j + 1, 8)]
            for jj, up in zip(range(j + 1, 8), ups):
                ctop[jj] = ctop[jj] - lt * up
            rows = rows - lt * rows[j : j + 1, :]
            if rest:
                ll = clow[j] * rec
                for jj, up in zip(range(j + 1, 8), ups):
                    clow[jj] = clow[jj] - ll * up
                llow.append(ll)
        m_ref[c0 : c0 + 8, :] = rows
        d_ref[c0 : c0 + 8, :] = dvec
        if rest:
            lanes = lax.broadcasted_iota(jnp.int32, (rest, W), 1)
            acc = jnp.where((lanes >= c0) & (lanes < c0 + 8), 0.0, low)
            for j in range(8):
                acc = acc - llow[j] * rows[j : j + 1, :]
            m_ref[c0 + 8 :, :] = acc
        for work in ticks.get(g, ()):
            work()


class Place:
    def __init__(self):
        self.g = lax.axis_index("grp")
        self.c = lax.axis_index("col")
        self.at = {"x": lax.rem(self.g, 4), "y": lax.div(self.g, 4), "z": lax.div(self.c, 2)}
        self.core = lax.rem(self.c, 2)
        self.partner = (self.g, self.at["z"] * 2 + 1 - self.core)

    def near(self, dim, delta):
        to = dict(self.at)
        to[dim] = lax.rem(self.at[dim] + delta + 4, 4)
        return (to["y"] * 4 + to["x"], to["z"] * 2 + self.core)

    def greet(self):
        barrier = pltpu.get_barrier_semaphore()
        peers = [self.near(d, s) for d in "xyz" for s in (1, 2, 3)] + [self.partner]
        for peer in peers:
            pl.semaphore_signal(barrier, inc=1, device_id=peer, device_id_type=MESH)
        pl.semaphore_wait(barrier, len(peers))


class Wires:
    def __init__(self, send, recv, count):
        self.send, self.recv, self.count, self.used = send, recv, count, 0

    def copy(self, ref, device):
        n = self.used
        self.used += 1
        assert n < self.count
        return pltpu.make_async_remote_copy(
            src_ref=ref,
            dst_ref=ref,
            send_sem=self.send.at[n],
            recv_sem=self.recv.at[n],
            device_id=device,
            device_id_type=MESH,
        )


def gather_stream(place, wires, view, order, rows, middle, across, direct):
    lo, hi = pl.ds(rows[0], middle - rows[0]), pl.ds(middle, rows[1] - middle)
    every = pl.ds(rows[0], rows[1] - rows[0])
    sent = []
    d2d = []

    def launch(copy, to=None):
        copy.start()
        sent.append(copy)
        if to is not None:
            to.append(copy)
        return copy

    for phase, dim in enumerate(order):
        last = across and phase == len(order) - 1

        def unit(v, r, dim=dim, phase=phase):
            where = {d: (FULL if d in order[:phase] else place.at[d]) for d in order}
            where[dim] = v
            return view(where, r)

        mine = place.at[dim]
        before, after, far = (lax.rem(mine + n, 4) for n in (3, 1, 2))
        right, left = place.near(dim, 1), place.near(dim, -1)
        to_right = launch(wires.copy(unit(mine, every), right))
        to_left = launch(wires.copy(unit(mine, every), left))
        if phase < direct:
            to_far = launch(wires.copy(unit(mine, every), place.near(dim, 2)))
            yield
            to_right.wait_recv()
            to_left.wait_recv()
            to_far.wait_recv()
            continue
        if last:
            launch(wires.copy(unit(mine, every), place.partner), d2d)
        yield
        to_right.wait_recv()
        on_right = launch(wires.copy(unit(before, lo), right))
        if last:
            launch(wires.copy(unit(before, every), place.partner), d2d)
        to_left.wait_recv()
        on_left = launch(wires.copy(unit(after, hi), left))
        if last:
            launch(wires.copy(unit(after, every), place.partner), d2d)
        yield
        on_right.wait_recv()
        on_left.wait_recv()
        if last:
            launch(wires.copy(unit(far, every), place.partner), d2d)
    yield
    for copy in d2d:
        copy.wait_recv()
    yield
    for copy in sent:
        copy.wait_send()


def straight_bcast(on, r, wires, whole, near, partner=None, other=None):
    legs = [wires.copy(whole, near(n)) for n in (1, 2, 3)]
    across = wires.copy(whole, partner) if partner is not None else None

    @pl.when(on & (r == 0))
    def _():
        for leg in (legs[1], legs[0], legs[2]):
            leg.start()
        if across is not None:
            across.start()

    yield
    for n in (1, 2, 3):

        @pl.when(on & (r == n))
        def _():
            legs[n - 1].wait_recv()
            if across is not None:
                across.start()

    if across is not None:
        yield

        @pl.when(other)
        def _():
            across.wait_recv()

        yield

        @pl.when(on)
        def _():
            across.wait_send()

    @pl.when(on & (r == 0))
    def _():
        for leg in legs:
            leg.wait_send()


def ring_bcast(on, r, wires, whole, lo, hi, right, left, partner=None, other=None):
    to_right, to_left = wires.copy(whole, right), wires.copy(whole, left)
    on_right, on_left = wires.copy(lo, right), wires.copy(hi, left)
    across = wires.copy(whole, partner) if partner is not None else None

    @pl.when(on & (r == 0))
    def _():
        to_right.start()
        to_left.start()
        if across is not None:
            across.start()

    yield

    @pl.when(on & (r == 1))
    def _():
        to_right.wait_recv()
        on_right.start()
        if across is not None:
            across.start()

    @pl.when(on & (r == 3))
    def _():
        to_left.wait_recv()
        on_left.start()
        if across is not None:
            across.start()

    yield

    @pl.when(on & (r == 2))
    def _():
        on_right.wait_recv()
        on_left.wait_recv()
        if across is not None:
            across.start()

    if across is not None:
        yield

        @pl.when(other)
        def _():
            across.wait_recv()

        yield

        @pl.when(on)
        def _():
            across.wait_send()

    @pl.when(on & (r == 0))
    def _():
        to_right.wait_send()
        to_left.wait_send()

    @pl.when(on & (r == 1))
    def _():
        on_right.wait_send()

    @pl.when(on & (r == 3))
    def _():
        on_left.wait_send()


class Round:
    def __init__(self, streams):
        self.streams = list(streams)

    def __call__(self):
        for s in self.streams:
            next(s, None)


TILES = ((3, 3, 2), (3, 2, 3), (2, 3, 3), (3, 3, 2))
ORDERS = ("xyz", "yzx", "zxy")
WIRES = 4 * 7 + 5 * 3 + 6 * 2 + 6 * 7 + 3 * 2 + 4 * 6 + 4 * 7 + 15 * 12
SLOTS = (5, 10, 15)


def panels_kernel(
    head_ref,
    child_ref,
    map_ref,
    flag_ref,
    all_ref,
    cg_ref,
    w_ref,
    maps_ref,
    own_ref,
    flead_ref,
    lead_ref,
    q_ref,
    coef_ref,
    m_ref,
    d_ref,
    rhs_ref,
    send_sem,
    recv_sem,
):
    place = Place()
    wires = Wires(send_sem, recv_sem, WIRES)
    x, y, z = place.at["x"], place.at["y"], place.at["z"]
    me = place.g * 8 + place.c
    low = place.c < PANELS
    row = lax.broadcasted_iota(jnp.int32, (W, W), 0)
    col = lax.broadcasted_iota(jnp.int32, (W, W), 1)

    entry = lax.broadcasted_iota(jnp.int32, (PACK, W), 0)
    packed = jnp.zeros((PACK, W), F32)
    for i in range(8):
        packed = jnp.where(entry == i, map_ref[0, i].astype(F32), packed)
    cg_ref[y, x, 0:PACK, :] = packed.astype(BF16)
    cg_ref[y, x, PACK:ROWS, :] = child_ref[0].astype(BF16)
    own_ref[...] = head_ref[...]
    for k in range(PANELS):

        @pl.when(me == k)
        def _():
            at = pl.ds(k * W, W)
            own_ref[at, :] += jnp.where(row == col, flag_ref[...].astype(F32), 0.0)

    @pl.when((place.g == 0) & low)
    def _():
        flead_ref[...] = own_ref[...]

    place.greet()

    def child_view(where, rows):
        return cg_ref.at[where["y"], where["x"], rows, :]

    def child_stream(r0, r1, order, direct=1):
        middle = r0 + (r1 - r0 + 16) // 32 * 16
        return gather_stream(place, wires, child_view, order, (r0, r1), middle, False, direct)

    def spread(j):
        first, second = ("x", "y") if j % 2 == 0 else ("y", "x")
        base = j * W
        half = W // 2
        refs = [flead_ref.at[pl.ds(at, size)] for at, size in ((base, W), (base, half), (base + half, half))]
        for dim, on in ((first, low & (place.at[second] == 0)), (second, low)):
            if j == 0:
                yield from straight_bcast(on, place.at[dim], wires, refs[0], lambda n, dim=dim: place.near(dim, n))
            else:
                yield from ring_bcast(on, place.at[dim], wires, *refs, place.near(dim, 1), place.near(dim, -1))

    def lead_unit(l, k):
        on = place.core == l % 2
        r = lax.rem(z - l // 2 + 4, 4)
        half = W // 2
        if k < 2:
            return straight_bcast(
                on, r, wires, lead_ref.at[l, k], lambda n: place.near("z", n), place.partner, place.core != l % 2
            )
        refs = [lead_ref.at[l, k], lead_ref.at[l, k, pl.ds(0, half)], lead_ref.at[l, k, pl.ds(half, half)]]
        return ring_bcast(
            on, r, wires, *refs, place.near("z", 1), place.near("z", -1), place.partner, place.core != l % 2
        )

    def panel_stream(k, p):
        def view(where, rows):
            return all_ref.at[k, where["y"], where["x"], where["z"], place.core, rows, :]

        r0 = 16 * sum(TILES[k][:p])
        n = TILES[k][p]
        half = (n // 2 if (k + p) % 2 else (n + 1) // 2) * 16
        return gather_stream(place, wires, view, ORDERS[p], (r0, r0 + 16 * n), r0 + half, True, 1)

    def first_row(s):
        return PACK + s * W if s else 0

    a = [
        Round(
            [
                child_stream(first_row(s), PACK + s * W + 64, "xy", 1 if s else 2),
                child_stream(PACK + s * W + 64, PACK + s * W + W, "yx", 1 if s else 2),
            ]
        )
        for s in range(PANELS)
    ]
    f = [Round([spread(s)]) for s in range(PANELS)]
    far = PACK + LEAD
    b = [
        Round([child_stream(far + n * W, far + (n + 1) * W, "xy" if n % 2 == 0 else "yx") for n in (m, m + 1)])
        for m in (0, 2)
    ]
    lead = [Round([lead_unit(l, k) for l in range(k, PANELS)]) for k in range(PANELS)]
    g = [Round([panel_stream(k, p) for p in range(3)]) for k in range(PANELS)]

    def assemble(k):
        at = pl.ds(k * W, W)
        acc_own, acc_lead = own_ref[at, :], flead_ref[at, :]
        for child in range(16):
            cy, cx = child // 4, child % 4
            names = cg_ref[cy, cx, 0:PACK, :].astype(F32)
            target = jnp.sum(jnp.where(entry == place.c, names, 0.0), axis=0, keepdims=True)
            here = names[k : k + 1, :] == float(k)
            mine = jnp.where((target == me.astype(F32)) & here, 1.0, 0.0)
            first = jnp.where((target == place.c.astype(F32)) & here, 1.0, 0.0)
            block = cg_ref[cy, cx, PACK + k * W : PACK + (k + 1) * W, :].astype(F32)
            acc_own = acc_own + block * mine
            acc_lead = acc_lead + block * first
            if k == 0:
                diagonal = lax.broadcasted_iota(jnp.int32, (PACK, W), 1) == entry
                line = jnp.sum(jnp.where(diagonal, names, 0.0), axis=0, keepdims=True)
                maps_ref[child : child + 1, :] = line.astype(jnp.int32)
        own_ref[at, :] = acc_own
        for l in range(k, PANELS):

            @pl.when(place.c == l)
            def _():
                lead_ref[l, k] = acc_lead

    def panel(k, plan):
        width = PANELS - 1 - k
        at = pl.ds(k * W, W)
        base = jnp.concatenate([lead_ref[l, k] for l in range(k, PANELS)] + [own_ref[at, :]], axis=1)
        if k:
            base = base - jnp.dot(
                coef_ref[k * W : (k + 1) * W, : k * W], q_ref[: k * W, k * W :], preferred_element_type=F32
            )
        diag = base[:, :W]
        diag = 0.5 * (diag + diag.T)
        m_ref[...] = diag
        rhs_ref[:, :W] = jnp.where(me == k, diag, base[:, (width + 1) * W :])
        if width:
            rhs_ref[:, W : W + width * W] = base[:, W : W + width * W]
        ldl_inverse(m_ref, d_ref, dict(zip(SLOTS, plan)))
        d = d_ref[...]
        minv = jnp.where(col <= row, m_ref[...], 0.0) / d
        piv = d.astype(BF16).astype(F32)
        rhs = rhs_ref[:, : W + width * W]
        q = jnp.dot(minv, rhs, precision=lax.Precision.HIGHEST, preferred_element_type=F32)
        own = jnp.where((me > k) | ((me == k) & (col >= row)), q[:, :W], 0.0).astype(BF16).astype(F32)
        all_ref[k, y, x, z, place.core] = own.T.astype(BF16)
        g[k]()
        w_ref[k * W : (k + 1) * W, :] = (own * piv).astype(BF16)
        q_ref[k * W : (k + 1) * W, LEAD:] = own.astype(BF16)
        for i in range(width):
            l = k + 1 + i
            part = q[:, (1 + i) * W : (2 + i) * W].astype(BF16)
            q_ref[k * W : (k + 1) * W, l * W : (l + 1) * W] = part
            coef_ref[l * W : (l + 1) * W, k * W : (k + 1) * W] = (
                (part.astype(F32) * piv).astype(BF16).astype(F32).T.astype(BF16)
            )

    def run(*rounds):
        for work in rounds:
            work()

    late = (1, 2, 3)

    def begin(k):
        assemble(k)
        lead[k]()

    run(a[0], f[0], *[a[k] for k in late], *[f[k] for k in late])
    run(a[0], f[0], *[f[k] for k in late], *[a[k] for k in late])
    run(a[0], f[0])
    begin(0)
    run(*[f[k] for k in late], b[0], b[1], lead[0], *[a[k] for k in late], lead[0])
    panel(
        0,
        (
            (*[f[k] for k in late], *[a[k] for k in late], f[1], lambda: begin(1)),
            (f[2], f[3], lambda: [begin(k) for k in (2, 3)], b[0], b[1]),
            (),
        ),
    )
    run(lead[1], lead[2], lead[3], lead[1])
    panel(1, ((b[0], b[1]), (lead[2], lead[3]), (lead[2], lead[3], g[0])))
    panel(2, ((b[0], b[1]), (g[0],), (g[1],)))
    panel(3, ((), (g[1],), (g[2], g[0])))
    run(g[1], g[3], g[2], g[0], g[3], g[2], g[1], g[3], g[0], g[2], g[1], g[3], g[0], g[2], g[3], g[1], g[2], g[3])
    for group in a + f + b + lead + g:
        for stream in group.streams:
            for _ in stream:
                pass
    assert wires.used == WIRES


def panels(head, contributions, block_map, flags):
    vmem = pl.BlockSpec(memory_space=pltpu.VMEM)
    return pl.pallas_call(
        panels_kernel,
        out_shape=(
            pltpu.VMEM((PANELS, 4, 4, 4, 2, W, W), BF16),
            pltpu.VMEM((4, 4, ROWS, W), BF16),
            pltpu.VMEM((LEAD, W), BF16),
            jax.ShapeDtypeStruct((16, W), jnp.int32),
        ),
        in_specs=[vmem, vmem, pl.BlockSpec(memory_space=pltpu.SMEM), vmem],
        out_specs=(vmem, vmem, vmem, vmem),
        scratch_shapes=[
            pltpu.VMEM((LEAD, W), F32),
            pltpu.VMEM((LEAD, W), F32),
            pltpu.VMEM((PANELS, PANELS, W, W), F32),
            pltpu.VMEM((LEAD, LEAD + W), BF16),
            pltpu.VMEM((LEAD, LEAD), BF16),
            pltpu.VMEM((W, W), F32),
            pltpu.VMEM((W, W), F32),
            pltpu.VMEM((W, LEAD), F32),
            pltpu.SemaphoreType.DMA((WIRES,)),
            pltpu.SemaphoreType.DMA((WIRES,)),
        ],
        compiler_params=pltpu.CompilerParams(
            collective_id=0, has_side_effects=True, vmem_limit_bytes=VMEM_PANELS
        ),
        cost_estimate=pl.CostEstimate(flops=2 * 10**10, bytes_accessed=3 * 2**20, transcendentals=0),
        name="panels",
    )(head, contributions, block_map, flags)


VMEM_PANELS = 12 * 2**20
VMEM_UPDATE = 12 * 2**20
CHUNK = 2048
SPAN = CHUNK // W


def update_kernel(me_ref, maps_ref, front_ref, l_ref, w_ref, parts_ref, flag_ref, out_ref, list_ref):
    s = pl.program_id(0)
    me = me_ref[0]
    groups = parts_ref.shape[0]
    rows = pl.ds(pl.multiple_of(s * CHUNK, CHUNK), CHUNK)

    @pl.when(s == 0)
    def _():
        count = jnp.int32(0)
        for g in range(groups):
            mine = maps_ref[g, lax.rem(me, 8)] == me
            list_ref[count] = g
            count = count + mine.astype(jnp.int32)
        list_ref[groups] = count

    @pl.when(me < PANELS)
    def _():
        out_ref[...] = l_ref[jnp.minimum(me, PANELS - 1), rows, :].astype(F32)

    @pl.when(me >= PANELS)
    def _():
        left = jnp.concatenate([l_ref[k, rows, :] for k in range(PANELS)], axis=1)
        out_ref[...] = front_ref[rows, :] - jnp.dot(left, w_ref[...], preferred_element_type=F32)

        def add(n, carry):
            g = list_ref[n]
            for i in range(8):
                block = maps_ref[g, i] - s * SPAN

                @pl.when((block >= 0) & (block < SPAN))
                def _():
                    at = pl.ds(pl.multiple_of(block * W, W), W)
                    out_ref[at, :] += parts_ref[g, PACK + i * W : PACK + (i + 1) * W, :].astype(F32)

            return carry

        lax.fori_loop(0, list_ref[groups], add, 0)

        @pl.when(lax.div(me, SPAN) == s)
        def _():
            at = pl.ds(pl.multiple_of(lax.rem(me, SPAN) * W, W), W)
            row = lax.broadcasted_iota(jnp.int32, (W, W), 0)
            col = lax.broadcasted_iota(jnp.int32, (W, W), 1)
            out_ref[at, :] += jnp.where(row == col, flag_ref[...].astype(F32), 0.0)

        @pl.when(s == 0)
        def _():
            out_ref[:LEAD, :] = jnp.zeros((LEAD, W), F32)


def update(me, maps, front, all_l, w, parts, flags):
    order = front.shape[0]
    vmem = pl.BlockSpec(memory_space=pltpu.VMEM)
    smem = pl.BlockSpec(memory_space=pltpu.SMEM)
    return pl.pallas_call(
        update_kernel,
        out_shape=jax.ShapeDtypeStruct((order, W), F32),
        grid=(order // CHUNK,),
        in_specs=[smem, smem, vmem, vmem, vmem, vmem, vmem],
        out_specs=pl.BlockSpec((CHUNK, W), lambda s: (s, 0)),
        scratch_shapes=[pltpu.SMEM((parts.shape[0] + 1,), jnp.int32)],
        compiler_params=pltpu.CompilerParams(vmem_limit_bytes=VMEM_UPDATE),
        name="update",
    )(me, maps, front, all_l, w, parts, flags)


def on_device(front, contributions, block_map, pivot_flags):
    which = lax.axis_index(("grp", "col")).reshape(1)
    flags = pivot_flags.reshape(1, W)
    all_l, parts, w, maps = panels(front[:LEAD], contributions, block_map, flags)
    all_l = all_l.reshape(PANELS, front.shape[0], W)
    return update(which, maps, front, all_l, w, parts.reshape(16, ROWS, W), flags)


def solution(mesh):
    return jax.shard_map(
        on_device,
        mesh=mesh,
        in_specs=(
            P(None, ("grp", "col")),
            P("grp", None, "col"),
            P("grp", None),
            P(("grp", "col")),
        ),
        out_specs=P(None, ("grp", "col")),
        check_vma=False,
    )
```

```python
import jax
import jax.numpy as jnp
from jax import lax
from jax.experimental import pallas as pl
from jax.experimental.pallas import tpu as pltpu
from jax.sharding import PartitionSpec as P

PANELS = 4
W = 128
LEAD = PANELS * W
PACK = 16
CHILD = 1024
ROWS = PACK + CHILD
MESH = pl.DeviceIdType.MESH
FULL = pl.ds(0, 4)
F32 = jnp.float32
BF16 = jnp.bfloat16


def ldl_inverse(m_ref, d_ref, ticks):
    lane = lax.broadcasted_iota(jnp.int32, (8, W), 1)
    sub = lax.broadcasted_iota(jnp.int32, (8, W), 0)
    for g in range(W // 8):
        c0 = 8 * g
        rest = W - c0 - 8
        top = m_ref[c0 : c0 + 8, :]
        ctop = [jnp.broadcast_to(top[:, c0 + j : c0 + j + 1], (8, W)) for j in range(8)]
        if rest:
            low = m_ref[c0 + 8 :, :]
            clow = [jnp.broadcast_to(low[:, c0 + j : c0 + j + 1], (rest, W)) for j in range(8)]
        inside = (lane >= c0) & (lane < c0 + 8)
        rows = jnp.where(inside, (lane == sub + c0).astype(F32), top)
        dvec = jnp.zeros((8, W), F32)
        llow = []
        for j in range(8):
            piv = ctop[j][j : j + 1, :]
            rec = 1.0 / piv
            dvec = jnp.where(sub == j, piv, dvec)
            lt = jnp.where(sub > j, ctop[j] * rec, 0.0)
            ups = [ctop[jj][j : j + 1, :] for jj in range(j + 1, 8)]
            for jj, up in zip(range(j + 1, 8), ups):
                ctop[jj] = ctop[jj] - lt * up
            rows = rows - lt * rows[j : j + 1, :]
            if rest:
                ll = clow[j] * rec
                for jj, up in zip(range(j + 1, 8), ups):
                    clow[jj] = clow[jj] - ll * up
                llow.append(ll)
        m_ref[c0 : c0 + 8, :] = rows
        d_ref[c0 : c0 + 8, :] = dvec
        if rest:
            lanes = lax.broadcasted_iota(jnp.int32, (rest, W), 1)
            acc = jnp.where((lanes >= c0) & (lanes < c0 + 8), 0.0, low)
            for j in range(8):
                acc = acc - llow[j] * rows[j : j + 1, :]
            m_ref[c0 + 8 :, :] = acc
        for work in ticks.get(g, ()):
            work()


class Place:
    def __init__(self):
        self.g = lax.axis_index("grp")
        self.c = lax.axis_index("col")
        self.at = {"x": lax.rem(self.g, 4), "y": lax.div(self.g, 4), "z": lax.div(self.c, 2)}
        self.core = lax.rem(self.c, 2)
        self.partner = (self.g, self.at["z"] * 2 + 1 - self.core)

    def near(self, dim, delta):
        to = dict(self.at)
        to[dim] = lax.rem(self.at[dim] + delta + 4, 4)
        return (to["y"] * 4 + to["x"], to["z"] * 2 + self.core)

    def greet(self):
        barrier = pltpu.get_barrier_semaphore()
        peers = [self.near(d, s) for d in "xyz" for s in (1, 2, 3)] + [self.partner]
        for peer in peers:
            pl.semaphore_signal(barrier, inc=1, device_id=peer, device_id_type=MESH)
        pl.semaphore_wait(barrier, len(peers))


class Wires:
    def __init__(self, send, recv, count):
        self.send, self.recv, self.count, self.used = send, recv, count, 0

    def copy(self, ref, device):
        n = self.used
        self.used += 1
        assert n < self.count
        return pltpu.make_async_remote_copy(
            src_ref=ref,
            dst_ref=ref,
            send_sem=self.send.at[n],
            recv_sem=self.recv.at[n],
            device_id=device,
            device_id_type=MESH,
        )


def gather_stream(place, wires, view, order, rows, middle, across, direct):
    lo, hi = pl.ds(rows[0], middle - rows[0]), pl.ds(middle, rows[1] - middle)
    every = pl.ds(rows[0], rows[1] - rows[0])
    sent = []
    d2d = []

    def launch(copy, to=None):
        copy.start()
        sent.append(copy)
        if to is not None:
            to.append(copy)
        return copy

    for phase, dim in enumerate(order):
        last = across and phase == len(order) - 1

        def unit(v, r, dim=dim, phase=phase):
            where = {d: (FULL if d in order[:phase] else place.at[d]) for d in order}
            where[dim] = v
            return view(where, r)

        mine = place.at[dim]
        before, after, far = (lax.rem(mine + n, 4) for n in (3, 1, 2))
        right, left = place.near(dim, 1), place.near(dim, -1)
        to_right = launch(wires.copy(unit(mine, every), right))
        to_left = launch(wires.copy(unit(mine, every), left))
        if phase < direct:
            to_far = launch(wires.copy(unit(mine, every), place.near(dim, 2)))
            yield
            to_right.wait_recv()
            to_left.wait_recv()
            to_far.wait_recv()
            continue
        if last:
            launch(wires.copy(unit(mine, every), place.partner), d2d)
        yield
        to_right.wait_recv()
        on_right = launch(wires.copy(unit(before, lo), right))
        if last:
            launch(wires.copy(unit(before, every), place.partner), d2d)
        to_left.wait_recv()
        on_left = launch(wires.copy(unit(after, hi), left))
        if last:
            launch(wires.copy(unit(after, every), place.partner), d2d)
        yield
        on_right.wait_recv()
        on_left.wait_recv()
        if last:
            launch(wires.copy(unit(far, every), place.partner), d2d)
    yield
    for copy in d2d:
        copy.wait_recv()
    yield
    for copy in sent:
        copy.wait_send()


def straight_bcast(on, r, wires, whole, near, partner=None, other=None):
    legs = [wires.copy(whole, near(n)) for n in (1, 2, 3)]
    across = wires.copy(whole, partner) if partner is not None else None

    @pl.when(on & (r == 0))
    def _():
        for leg in (legs[1], legs[0], legs[2]):
            leg.start()
        if across is not None:
            across.start()

    yield
    for n in (1, 2, 3):

        @pl.when(on & (r == n))
        def _():
            legs[n - 1].wait_recv()
            if across is not None:
                across.start()

    if across is not None:
        yield

        @pl.when(other)
        def _():
            across.wait_recv()

        yield

        @pl.when(on)
        def _():
            across.wait_send()

    @pl.when(on & (r == 0))
    def _():
        for leg in legs:
            leg.wait_send()


def ring_bcast(on, r, wires, whole, lo, hi, right, left, partner=None, other=None):
    to_right, to_left = wires.copy(whole, right), wires.copy(whole, left)
    on_right, on_left = wires.copy(lo, right), wires.copy(hi, left)
    across = wires.copy(whole, partner) if partner is not None else None

    @pl.when(on & (r == 0))
    def _():
        to_right.start()
        to_left.start()
        if across is not None:
            across.start()

    yield

    @pl.when(on & (r == 1))
    def _():
        to_right.wait_recv()
        on_right.start()
        if across is not None:
            across.start()

    @pl.when(on & (r == 3))
    def _():
        to_left.wait_recv()
        on_left.start()
        if across is not None:
            across.start()

    yield

    @pl.when(on & (r == 2))
    def _():
        on_right.wait_recv()
        on_left.wait_recv()
        if across is not None:
            across.start()

    if across is not None:
        yield

        @pl.when(other)
        def _():
            across.wait_recv()

        yield

        @pl.when(on)
        def _():
            across.wait_send()

    @pl.when(on & (r == 0))
    def _():
        to_right.wait_send()
        to_left.wait_send()

    @pl.when(on & (r == 1))
    def _():
        on_right.wait_send()

    @pl.when(on & (r == 3))
    def _():
        on_left.wait_send()


class Round:
    def __init__(self, streams):
        self.streams = list(streams)

    def __call__(self):
        for s in self.streams:
            next(s, None)


TILES = ((3, 3, 2), (3, 2, 3), (2, 3, 3), (3, 3, 2))
ORDERS = ("xyz", "yzx", "zxy")
WIRES = 4 * 7 + 5 * 3 + 6 * 2 + 6 * 7 + 3 * 2 + 4 * 6 + 4 * 7 + 15 * 12
SLOTS = (5, 10, 15)


def panels_kernel(
    head_ref,
    child_ref,
    map_ref,
    flag_ref,
    all_ref,
    cg_ref,
    w_ref,
    maps_ref,
    own_ref,
    flead_ref,
    lead_ref,
    q_ref,
    coef_ref,
    m_ref,
    d_ref,
    rhs_ref,
    send_sem,
    recv_sem,
):
    place = Place()
    wires = Wires(send_sem, recv_sem, WIRES)
    x, y, z = place.at["x"], place.at["y"], place.at["z"]
    me = place.g * 8 + place.c
    low = place.c < PANELS
    row = lax.broadcasted_iota(jnp.int32, (W, W), 0)
    col = lax.broadcasted_iota(jnp.int32, (W, W), 1)

    entry = lax.broadcasted_iota(jnp.int32, (PACK, W), 0)
    packed = jnp.zeros((PACK, W), F32)
    for i in range(8):
        packed = jnp.where(entry == i, map_ref[0, i].astype(F32), packed)
    cg_ref[y, x, 0:PACK, :] = packed.astype(BF16)
    cg_ref[y, x, PACK:ROWS, :] = child_ref[0].astype(BF16)
    own_ref[...] = head_ref[...]
    for k in range(PANELS):

        @pl.when(me == k)
        def _():
            at = pl.ds(k * W, W)
            own_ref[at, :] += jnp.where(row == col, flag_ref[...].astype(F32), 0.0)

    @pl.when((place.g == 0) & low)
    def _():
        flead_ref[...] = own_ref[...]

    place.greet()

    def child_view(where, rows):
        return cg_ref.at[where["y"], where["x"], rows, :]

    def child_stream(r0, r1, order, direct=1):
        middle = r0 + (r1 - r0 + 16) // 32 * 16
        return gather_stream(place, wires, child_view, order, (r0, r1), middle, False, direct)

    def spread(j):
        first, second = ("x", "y") if j % 2 == 0 else ("y", "x")
        base = j * W
        half = W // 2
        refs = [flead_ref.at[pl.ds(at, size)] for at, size in ((base, W), (base, half), (base + half, half))]
        for dim, on in ((first, low & (place.at[second] == 0)), (second, low)):
            if j == 0:
                yield from straight_bcast(on, place.at[dim], wires, refs[0], lambda n, dim=dim: place.near(dim, n))
            else:
                yield from ring_bcast(on, place.at[dim], wires, *refs, place.near(dim, 1), place.near(dim, -1))

    def lead_unit(l, k):
        on = place.core == l % 2
        r = lax.rem(z - l // 2 + 4, 4)
        half = W // 2
        if k < 2:
            return straight_bcast(
                on, r, wires, lead_ref.at[l, k], lambda n: place.near("z", n), place.partner, place.core != l % 2
            )
        refs = [lead_ref.at[l, k], lead_ref.at[l, k, pl.ds(0, half)], lead_ref.at[l, k, pl.ds(half, half)]]
        return ring_bcast(
            on, r, wires, *refs, place.near("z", 1), place.near("z", -1), place.partner, place.core != l % 2
        )

    def panel_stream(k, p):
        def view(where, rows):
            return all_ref.at[k, where["y"], where["x"], where["z"], place.core, rows, :]

        r0 = 16 * sum(TILES[k][:p])
        n = TILES[k][p]
        half = (n // 2 if (k + p) % 2 else (n + 1) // 2) * 16
        return gather_stream(place, wires, view, ORDERS[p], (r0, r0 + 16 * n), r0 + half, True, 1)

    def first_row(s):
        return PACK + s * W if s else 0

    a = [
        Round(
            [
                child_stream(first_row(s), PACK + s * W + 64, "xy", 1 if s else 2),
                child_stream(PACK + s * W + 64, PACK + s * W + W, "yx", 1 if s else 2),
            ]
        )
        for s in range(PANELS)
    ]
    f = [Round([spread(s)]) for s in range(PANELS)]
    far = PACK + LEAD
    b = [
        Round([child_stream(far + n * W, far + (n + 1) * W, "xy" if n % 2 == 0 else "yx") for n in (m, m + 1)])
        for m in (0, 2)
    ]
    lead = [Round([lead_unit(l, k) for l in range(k, PANELS)]) for k in range(PANELS)]
    g = [Round([panel_stream(k, p) for p in range(3)]) for k in range(PANELS)]

    def assemble(k):
        at = pl.ds(k * W, W)
        acc_own, acc_lead = own_ref[at, :], flead_ref[at, :]
        for child in range(16):
            cy, cx = child // 4, child % 4
            names = cg_ref[cy, cx, 0:PACK, :].astype(F32)
            target = jnp.sum(jnp.where(entry == place.c, names, 0.0), axis=0, keepdims=True)
            here = names[k : k + 1, :] == float(k)
            mine = jnp.where((target == me.astype(F32)) & here, 1.0, 0.0)
            first = jnp.where((target == place.c.astype(F32)) & here, 1.0, 0.0)
            block = cg_ref[cy, cx, PACK + k * W : PACK + (k + 1) * W, :].astype(F32)
            acc_own = acc_own + block * mine
            acc_lead = acc_lead + block * first
            if k == 0:
                diagonal = lax.broadcasted_iota(jnp.int32, (PACK, W), 1) == entry
                line = jnp.sum(jnp.where(diagonal, names, 0.0), axis=0, keepdims=True)
                maps_ref[child : child + 1, :] = line.astype(jnp.int32)
        own_ref[at, :] = acc_own
        for l in range(k, PANELS):

            @pl.when(place.c == l)
            def _():
                lead_ref[l, k] = acc_lead

    def panel(k, plan):
        width = PANELS - 1 - k
        at = pl.ds(k * W, W)
        base = jnp.concatenate([lead_ref[l, k] for l in range(k, PANELS)] + [own_ref[at, :]], axis=1)
        if k:
            base = base - jnp.dot(
                coef_ref[k * W : (k + 1) * W, : k * W], q_ref[: k * W, k * W :], preferred_element_type=F32
            )
        diag = base[:, :W]
        diag = 0.5 * (diag + diag.T)
        m_ref[...] = diag
        rhs_ref[:, :W] = jnp.where(me == k, diag, base[:, (width + 1) * W :])
        if width:
            rhs_ref[:, W : W + width * W] = base[:, W : W + width * W]
        ldl_inverse(m_ref, d_ref, dict(zip(SLOTS, plan)))
        d = d_ref[...]
        minv = jnp.where(col <= row, m_ref[...], 0.0) / d
        piv = d.astype(BF16).astype(F32)
        rhs = rhs_ref[:, : W + width * W]
        q = jnp.dot(minv, rhs, precision=lax.Precision.HIGHEST, preferred_element_type=F32)
        own = jnp.where((me > k) | ((me == k) & (col >= row)), q[:, :W], 0.0).astype(BF16).astype(F32)
        all_ref[k, y, x, z, place.core] = own.T.astype(BF16)
        g[k]()
        w_ref[k * W : (k + 1) * W, :] = (own * piv).astype(BF16)
        q_ref[k * W : (k + 1) * W, LEAD:] = own.astype(BF16)
        for i in range(width):
            l = k + 1 + i
            part = q[:, (1 + i) * W : (2 + i) * W].astype(BF16)
            q_ref[k * W : (k + 1) * W, l * W : (l + 1) * W] = part
            coef_ref[l * W : (l + 1) * W, k * W : (k + 1) * W] = (
                (part.astype(F32) * piv).astype(BF16).astype(F32).T.astype(BF16)
            )

    def run(*rounds):
        for work in rounds:
            work()

    late = (1, 2, 3)

    def begin(k):
        assemble(k)
        lead[k]()

    run(a[0], f[0], *[a[k] for k in late], *[f[k] for k in late])
    run(a[0], f[0], *[f[k] for k in late], *[a[k] for k in late])
    run(a[0], f[0])
    begin(0)
    run(*[f[k] for k in late], b[0], b[1], lead[0], *[a[k] for k in late], lead[0])
    panel(
        0,
        (
            (*[f[k] for k in late], *[a[k] for k in late], f[1], lambda: begin(1)),
            (f[2], f[3], lambda: [begin(k) for k in (2, 3)], b[0], b[1]),
            (),
        ),
    )
    run(lead[1], lead[2], lead[3], lead[1])
    panel(1, ((b[0], b[1]), (lead[2], lead[3]), (lead[2], lead[3], g[0])))
    panel(2, ((b[0], b[1]), (g[0],), (g[1],)))
    panel(3, ((), (g[1],), (g[2], g[0])))
    run(g[1], g[3], g[2], g[0], g[3], g[2], g[1], g[3], g[0], g[2], g[1], g[3], g[0], g[2], g[3], g[1], g[2], g[3])
    for group in a + f + b + lead + g:
        for stream in group.streams:
            for _ in stream:
                pass
    assert wires.used == WIRES


def panels(head, contributions, block_map, flags):
    vmem = pl.BlockSpec(memory_space=pltpu.VMEM)
    return pl.pallas_call(
        panels_kernel,
        out_shape=(
            pltpu.VMEM((PANELS, 4, 4, 4, 2, W, W), BF16),
            pltpu.VMEM((4, 4, ROWS, W), BF16),
            pltpu.VMEM((LEAD, W), BF16),
            jax.ShapeDtypeStruct((16, W), jnp.int32),
        ),
        in_specs=[vmem, vmem, pl.BlockSpec(memory_space=pltpu.SMEM), vmem],
        out_specs=(vmem, vmem, vmem, vmem),
        scratch_shapes=[
            pltpu.VMEM((LEAD, W), F32),
            pltpu.VMEM((LEAD, W), F32),
            pltpu.VMEM((PANELS, PANELS, W, W), F32),
            pltpu.VMEM((LEAD, LEAD + W), BF16),
            pltpu.VMEM((LEAD, LEAD), BF16),
            pltpu.VMEM((W, W), F32),
            pltpu.VMEM((W, W), F32),
            pltpu.VMEM((W, LEAD), F32),
            pltpu.SemaphoreType.DMA((WIRES,)),
            pltpu.SemaphoreType.DMA((WIRES,)),
        ],
        compiler_params=pltpu.CompilerParams(
            collective_id=0, has_side_effects=True, vmem_limit_bytes=VMEM_PANELS
        ),
        cost_estimate=pl.CostEstimate(flops=2 * 10**10, bytes_accessed=3 * 2**20, transcendentals=0),
        name="panels",
    )(head, contributions, block_map, flags)


VMEM_PANELS = 12 * 2**20
VMEM_UPDATE = 16 * 2**20
CHUNK = 4096
SPAN = CHUNK // W


def update_kernel(me_ref, maps_ref, front_ref, l_ref, w_ref, parts_ref, flag_ref, out_ref, list_ref):
    s = pl.program_id(0)
    me = me_ref[0]
    groups = parts_ref.shape[0]
    rows = pl.ds(pl.multiple_of(s * CHUNK, CHUNK), CHUNK)

    @pl.when(s == 0)
    def _():
        count = jnp.int32(0)
        for g in range(groups):
            mine = maps_ref[g, lax.rem(me, 8)] == me
            list_ref[count] = g
            count = count + mine.astype(jnp.int32)
        list_ref[groups] = count

    @pl.when(me < PANELS)
    def _():
        out_ref[...] = l_ref[jnp.minimum(me, PANELS - 1), rows, :].astype(F32)

    @pl.when(me >= PANELS)
    def _():
        left = jnp.concatenate([l_ref[k, rows, :] for k in range(PANELS)], axis=1)
        out_ref[...] = front_ref[rows, :] - jnp.dot(left, w_ref[...], preferred_element_type=F32)

        def add(n, carry):
            g = list_ref[n]
            for i in range(8):
                block = maps_ref[g, i] - s * SPAN

                @pl.when((block >= 0) & (block < SPAN))
                def _():
                    at = pl.ds(pl.multiple_of(block * W, W), W)
                    out_ref[at, :] += parts_ref[g, PACK + i * W : PACK + (i + 1) * W, :].astype(F32)

            return carry

        lax.fori_loop(0, list_ref[groups], add, 0)

        @pl.when(lax.div(me, SPAN) == s)
        def _():
            at = pl.ds(pl.multiple_of(lax.rem(me, SPAN) * W, W), W)
            row = lax.broadcasted_iota(jnp.int32, (W, W), 0)
            col = lax.broadcasted_iota(jnp.int32, (W, W), 1)
            out_ref[at, :] += jnp.where(row == col, flag_ref[...].astype(F32), 0.0)

        @pl.when(s == 0)
        def _():
            out_ref[:LEAD, :] = jnp.zeros((LEAD, W), F32)


def update(me, maps, front, all_l, w, parts, flags):
    order = front.shape[0]
    vmem = pl.BlockSpec(memory_space=pltpu.VMEM)
    smem = pl.BlockSpec(memory_space=pltpu.SMEM)
    return pl.pallas_call(
        update_kernel,
        out_shape=jax.ShapeDtypeStruct((order, W), F32),
        grid=(order // CHUNK,),
        in_specs=[smem, smem, vmem, vmem, vmem, vmem, vmem],
        out_specs=pl.BlockSpec((CHUNK, W), lambda s: (s, 0)),
        scratch_shapes=[pltpu.SMEM((parts.shape[0] + 1,), jnp.int32)],
        compiler_params=pltpu.CompilerParams(vmem_limit_bytes=VMEM_UPDATE),
        name="update",
    )(me, maps, front, all_l, w, parts, flags)


def on_device(front, contributions, block_map, pivot_flags):
    which = lax.axis_index(("grp", "col")).reshape(1)
    flags = pivot_flags.reshape(1, W)
    all_l, parts, w, maps = panels(front[:LEAD], contributions, block_map, flags)
    all_l = all_l.reshape(PANELS, front.shape[0], W)
    return update(which, maps, front, all_l, w, parts.reshape(16, ROWS, W), flags)


def solution(mesh):
    return jax.shard_map(
        on_device,
        mesh=mesh,
        in_specs=(
            P(None, ("grp", "col")),
            P("grp", None, "col"),
            P("grp", None),
            P(("grp", "col")),
        ),
        out_specs=P(None, ("grp", "col")),
        check_vma=False,
    )
```
